32 devices in a mesh: dp: 1 (over z), ep: 32 (over y, x, core).
Axes of the slice: x: 4, y: 4, z: 1, core: 2. Of those that a mesh axis runs over, the one named last changes fastest.
The devices are a block of a 4x4x8 slice.
Arguments:
- tokens: bfloat16 [2048, 2048], P(('dp', 'ep'))
- routes: int32 [2048, 8], P(('dp', 'ep'))
- w_router: bfloat16 [2048, 128], replicated
- w_one: bfloat16 [128, 2048, 768], P('ep')
- w_three: bfloat16 [128, 2048, 768], P('ep')
- w_two: bfloat16 [128, 768, 2048], P('ep')
Outputs:
- output: bfloat16 [2048, 2048], P(('dp', 'ep'))
All inputs are finite; a program needn't handle non-finite values.
Results may differ from the reference program's by a relative error of at most 0.00819039.
Values are sent between devices in bfloat16 or wider.
A program may use at most 768 MiB of HBM per device.

```python
import jax
import jax.numpy as jnp
from jax import lax

GROUP_SIZE = 32
DEV_TOKENS = 64
D_MODEL = 2048
D_EXPERT = 768
NUM_EXPERTS = 128
TOP_K = 8
CAPACITY = 8


def draw_routes(route_key):
    perm_key, row_key, slot_key = jax.random.split(route_key, 3)
    num_pairs = DEV_TOKENS * TOP_K
    hot_count = NUM_EXPERTS // 8
    rest_pairs = num_pairs - hot_count * CAPACITY
    base_count = rest_pairs // (NUM_EXPERTS - hot_count)
    extra_count = rest_pairs % (NUM_EXPERTS - hot_count)
    rank_ids = jnp.arange(NUM_EXPERTS, dtype=jnp.int32)
    counts = jnp.where(rank_ids < hot_count, CAPACITY, base_count + (rank_ids - hot_count < extra_count).astype(jnp.int32))
    count_ends = jnp.cumsum(counts)
    pair_rank = jnp.searchsorted(count_ends, jnp.arange(num_pairs, dtype=jnp.int32), side='right')
    expert_of_rank = jax.random.permutation(perm_key, NUM_EXPERTS)
    layout = expert_of_rank[pair_rank].reshape(TOP_K, DEV_TOKENS).T

    def device_routes(perm_rows, perm_slots):
        row_order = jax.random.permutation(perm_rows, DEV_TOKENS)
        scores = jax.random.randint(perm_slots, (DEV_TOKENS, TOP_K), 0, 1 << 20) * TOP_K + jnp.arange(TOP_K)
        slot_order = jnp.argsort(scores, axis=1)
        return jnp.take_along_axis(layout[row_order], slot_order, axis=1)

    per_device = jax.vmap(device_routes)(jax.random.split(row_key, GROUP_SIZE), jax.random.split(slot_key, GROUP_SIZE))
    return per_device.reshape(GROUP_SIZE * DEV_TOKENS, TOP_K).astype(jnp.int32)


def setup_inputs(seed: int = 0, part: int = 0) -> dict:
    part_key = jax.random.fold_in(jax.random.key(seed), part)
    token_key, route_key = jax.random.split(part_key)
    shared = jax.random.split(jax.random.key(seed + 1), 4)
    tokens = jax.random.normal(token_key, (GROUP_SIZE * DEV_TOKENS, D_MODEL), jnp.float32)
    w_router = jax.random.normal(shared[0], (D_MODEL, NUM_EXPERTS), jnp.float32) * (1.5 * D_MODEL ** -0.5)
    w_one = jax.random.normal(shared[1], (NUM_EXPERTS, D_MODEL, D_EXPERT), jnp.float32) * D_MODEL ** -0.5
    w_three = jax.random.normal(shared[2], (NUM_EXPERTS, D_MODEL, D_EXPERT), jnp.float32) * D_MODEL ** -0.5
    w_two = jax.random.normal(shared[3], (NUM_EXPERTS, D_EXPERT, D_MODEL), jnp.float32) * D_EXPERT ** -0.5
    return {'tokens': tokens.astype(jnp.bfloat16), 'routes': draw_routes(route_key), 'w_router': w_router.astype(jnp.bfloat16), 'w_one': w_one.astype(jnp.bfloat16), 'w_three': w_three.astype(jnp.bfloat16), 'w_two': w_two.astype(jnp.bfloat16)}


def expert_rows(rows, w_gate, w_up, w_down):
    gate_pre = jnp.dot(rows, w_gate, preferred_element_type=jnp.float32)
    up_pre = jnp.dot(rows, w_up, preferred_element_type=jnp.float32)
    hidden = (jax.nn.silu(gate_pre) * up_pre).astype(jnp.bfloat16)
    return jnp.dot(hidden, w_down, preferred_element_type=jnp.float32).astype(jnp.bfloat16)


def reference(tokens, routes, w_router, w_one, w_three, w_two):
    logits = jnp.dot(tokens, w_router, preferred_element_type=jnp.float32)
    gate_vals = jax.nn.softmax(jnp.take_along_axis(logits, routes, axis=1), axis=-1)
    flat_gates = gate_vals.reshape(-1)
    flat_routes = routes.reshape(-1)
    num_pairs = flat_routes.shape[0]
    sort_order = jnp.argsort(flat_routes, stable=True)
    counts = jax.ops.segment_sum(jnp.ones_like(flat_routes), flat_routes, num_segments=NUM_EXPERTS)
    starts = jnp.cumsum(counts) - counts
    slot_ids = jnp.arange(GROUP_SIZE * CAPACITY, dtype=jnp.int32)

    def one_expert(y_sum, step_in):
        w_gate, w_up, w_down, exp_start, exp_count = step_in
        pair_at = sort_order[jnp.minimum(exp_start + slot_ids, num_pairs - 1)]
        token_at = pair_at // TOP_K
        weight = jnp.where(slot_ids < exp_count, flat_gates[pair_at], 0.0)
        out_rows = expert_rows(tokens[token_at], w_gate, w_up, w_down)
        return y_sum.at[token_at].add(weight[:, None] * out_rows.astype(jnp.float32)), None

    y_sum = lax.scan(one_expert, jnp.zeros(tokens.shape, jnp.float32), (w_one, w_three, w_two, starts, counts))[0]
    return y_sum.astype(jnp.bfloat16)
```

```python
import functools
import math

import jax
import jax.numpy as jnp
from jax import lax
from jax.experimental import pallas as pl
from jax.experimental.pallas import tpu as pltpu
from jax.sharding import PartitionSpec as P

MESH = pl.DeviceIdType.MESH
F32 = jnp.float32
BF16 = jnp.bfloat16
CORES = 2
LANES = 128


def slot_capacity(num_tokens, top_k, num_experts):
    return 8 * ((3 * num_tokens * top_k + 16 * num_experts - 1) // (16 * num_experts))


def moe_kernel(
    side,
    x_hbm, routes_ref, wr_hbm, w1_hbm, w3_hbm, w2_hbm, y_ref,
    xg, wr, w1, w3, w2, xo, hid, meta, slots, gates, mbuf, pbuf, ybuf,
    x_sem, wr_sem, w_sem, meta_ssem, meta_rsem, first_ssem, second_ssem, relay_ssem, core_ssem, ag_rsem, r1_ssem, r1_rsem, r2_ssem, r2_rsem,
):
    num_devices = CORES * side * side
    chips = side * side
    num_tokens, d_model = x_hbm.shape
    half = d_model // 2
    quarter = half // CORES
    local_experts = w1.shape[0]
    d_expert = w1.shape[2]
    chip_experts = CORES * local_experts
    num_experts = num_devices * local_experts
    top_k = routes_ref.shape[0]
    cap = xo.shape[3] // CORES

    me = lax.axis_index('ep')
    core = lax.rem(me, CORES)
    my_x = lax.rem(lax.div(me, CORES), side)
    my_y = lax.div(me, CORES * side)

    def ring(v, k):
        return lax.rem(v + k, side)

    def chip_at(y, x):
        return y * side + x

    def dev(y, x, c):
        return chip_at(y, x) * CORES + c

    partner = dev(my_y, my_x, 1 - core)

    def remote(src, dst, ssem, rsem, target):
        return pltpu.make_async_remote_copy(src_ref=src, dst_ref=dst, send_sem=ssem, recv_sem=rsem, device_id={'ep': target}, device_id_type=MESH)

    x_copies = [pltpu.make_async_copy(x_hbm.at[:, pl.ds(h * half, half)], xg.at[h, me], x_sem.at[h]) for h in range(2)]
    for cp in x_copies:
        cp.start()
    wr_copy = pltpu.make_async_copy(wr_hbm, wr, wr_sem.at[0])
    wr_copy.start()

    def weight_copies(e):
        return [pltpu.make_async_copy(src.at[e], dst.at[e], w_sem.at[i, e]) for i, (src, dst) in enumerate(((w1_hbm, w1), (w3_hbm, w3), (w2_hbm, w2)))]

    def start_weights(e, carry):
        for cp in weight_copies(e):
            cp.start()
        return carry

    lax.fori_loop(0, local_experts, start_weights, 0)

    barrier = pltpu.get_barrier_semaphore()

    def greet(i, carry):
        pl.semaphore_signal(barrier, inc=1, device_id={'ep': lax.rem(me + i, num_devices)}, device_id_type=MESH)
        return carry

    lax.fori_loop(1, num_devices, greet, 0)
    pl.semaphore_wait(barrier, num_devices - 1)
    for cp in x_copies:
        cp.wait()

    def place(h, a, b):
        if h == 0:
            return ring(my_y, b), ring(my_x, a)
        return ring(my_y, a), ring(my_x, b)

    def block_src(h, a, b, c):
        y, x = place(h, a, b)
        return dev(y, x, c)

    def move_block(h, src, ssem, target):
        return remote(xg.at[h, src], xg.at[h, src], ssem, ag_rsem.at[h, src], target)

    def wait_block(h, src):
        pltpu.make_async_copy(xg.at[h, src], xg.at[h, src], ag_rsem.at[h, src]).wait()

    def first_copy(h, k):
        return move_block(h, me, first_ssem.at[h, k], block_src(h, k, 0, core))

    def second_copy(h, a, k):
        return move_block(h, block_src(h, a, 0, core), second_ssem.at[h, a, k], block_src(h, 0, k, core))

    def relay_copy(h, a, k):
        return move_block(h, block_src(h, a, k, core), relay_ssem.at[h, a], block_src(h, 0, side - k, core))

    def core_copy(h, a, b):
        return move_block(h, block_src(h, a, b, core), core_ssem.at[h, a, b], partner)

    for h in range(2):
        for k in (1, side - 1) + tuple(range(2, side - 1)):
            first_copy(h, k).start()
        for k in (1, side - 1):
            second_copy(h, 0, k).start()
        core_copy(h, 0, 0).start()

    wr_copy.wait()
    x_local = [xg[h, me] for h in range(2)]
    logits = sum(
        lax.dot_general(wr[pl.ds(h * half, half), :], x_local[h], (((0,), (1,)), ((), ())), preferred_element_type=F32)
        for h in range(2)
    )
    routes = routes_ref[...]
    expert_iota = lax.broadcasted_iota(jnp.int32, (num_experts, num_tokens), 0)
    picked = jnp.concatenate(
        [jnp.sum(jnp.where(expert_iota == routes[j:j + 1, :], logits, 0.0), axis=0, keepdims=True) for j in range(top_k)], axis=0)
    ex = jnp.exp(picked - jnp.max(picked, axis=0, keepdims=True))
    gate = ex / jnp.sum(ex, axis=0, keepdims=True)
    tile = jnp.concatenate([routes.astype(F32) + 1.0, gate], axis=0)
    lane = lax.broadcasted_iota(jnp.int32, (2 * top_k, LANES), 1)
    meta[me] = jnp.where(lane // num_tokens == core, jnp.concatenate([tile] * CORES, axis=1), 0.0)

    def meta_copy(i):
        return remote(meta.at[me], meta.at[me], meta_ssem.at[i], meta_rsem.at[me], lax.rem(me + i, num_devices))

    def send_meta(i, carry):
        meta_copy(i).start()
        return carry

    def recv_meta(i, carry):
        src = lax.rem(me + i, num_devices)
        pltpu.make_async_copy(meta.at[src], meta.at[src], meta_rsem.at[src]).wait()
        return carry

    def sent_meta(i, carry):
        meta_copy(i).wait_send()
        return carry

    lax.fori_loop(1, num_devices, send_meta, 0)
    lax.fori_loop(1, num_devices, recv_meta, 0)

    row_i = lax.broadcasted_iota(jnp.int32, (LANES, LANES), 0)
    col_i = lax.broadcasted_iota(jnp.int32, (LANES, LANES), 1)
    before = jnp.where((row_i < col_i) & (row_i // num_tokens == col_i // num_tokens), 1.0, 0.0).astype(BF16)
    ids = lax.broadcasted_iota(jnp.int32, (num_experts, LANES), 0).astype(F32) + 1.0

    def plan_chip(p, carry):
        both = meta[CORES * p] + meta[CORES * p + 1]
        mask = jnp.zeros((num_experts, LANES), F32)
        weight = jnp.zeros((num_experts, LANES), F32)
        for j in range(top_k):
            hit = ids == both[j:j + 1, :]
            mask = jnp.where(hit, 1.0, mask)
            weight = jnp.where(hit, both[top_k + j:top_k + j + 1, :], weight)
        rank = jnp.dot(mask.astype(BF16), before, preferred_element_type=F32)
        slots[p] = jnp.where(mask > 0.0, rank, -1.0)
        gates[p] = weight
        return carry

    lax.fori_loop(0, chips, plan_chip, 0)

    pair_row = lax.broadcasted_iota(jnp.int32, (CORES * cap, LANES), 0)
    pair_lane = lax.broadcasted_iota(jnp.int32, (CORES * cap, LANES), 1)
    wanted = jnp.where(pair_row // cap == pair_lane // num_tokens, pair_row % cap, -2).astype(F32)

    def gather_chip(h, y, x):
        p = chip_at(y, x)
        mine = slots[p, pl.ds(me * local_experts, local_experts), :]
        pick = jnp.where(mine[:, None, :] == wanted[None], 1.0, 0.0).reshape(local_experts * CORES * cap, LANES).astype(BF16)
        rows = xg[h, pl.ds(p * CORES, CORES)].reshape(CORES * num_tokens, half)
        out = jnp.dot(pick, rows, preferred_element_type=F32).astype(BF16)
        xo[:, y, x, :, pl.ds(h * half, half)] = out.reshape(local_experts, CORES * cap, half)

    def finish(a, b):
        for h in range(2):
            wait_block(h, block_src(h, a, b, 1 - core))
            gather_chip(h, *place(h, a, b))

    def land(h, a, b):
        wait_block(h, block_src(h, a, b, core))
        core_copy(h, a, b).start()

    far = side // 2
    near = (1, side - 1) + tuple(range(2, side - 1))

    def same_line(a, carry):
        for h in range(2):
            land(h, a, 0)
            for k in (1, side - 1):
                second_copy(h, a, k).start()
        return carry

    def next_lines(a, carry):
        for h in range(2):
            land(h, a, 1)
            relay_copy(h, a, 1).start()
            land(h, a + far, side - 1)
            relay_copy(h, a + far, side - 1).start()
            land(h, a + far, 1)
            land(h, a, side - 1)
        finish(a, 0)
        finish(a + far, 0)
        return carry

    def far_line(a, carry):
        for h in range(2):
            land(h, a, far)
        finish(a, 1)
        finish(a, side - 1)
        return carry

    def last_blocks(a, carry):
        finish(a, far)
        return carry

    lax.fori_loop(1, side, same_line, 0)
    lax.fori_loop(0, far, next_lines, 0)
    lax.fori_loop(0, side, far_line, 0)
    lax.fori_loop(0, side, last_blocks, 0)

    def r1_place(h, k):
        if h == 0:
            return ring(my_y, k), my_x
        return my_y, ring(my_x, k)

    def r1_src(h, e, k, cm):
        y, x = r1_place(h, k)
        cols = pl.ds(h * half + cm * quarter, quarter)
        if h == 0:
            return xo.at[e, y, :, :, cols]
        return xo.at[e, :, x, :, cols]

    def r1_copy(h, e, k, cm):
        y, x = r1_place(h, k)
        return remote(r1_src(h, e, k, cm), mbuf.at[h, k, core, e], r1_ssem.at[h, k, cm, e], r1_rsem.at[h, k, core, e], dev(y, x, cm))

    def r1_partner(h, e):
        y, x = my_y, my_x
        cols = pl.ds(pl.multiple_of(h * half + (1 - core) * quarter, quarter), quarter)
        src = xo.at[e, y, :, :, cols] if h == 0 else xo.at[e, :, x, :, cols]
        return remote(src, mbuf.at[h, 0, core, e], r1_ssem.at[h, 0, 0, e], r1_rsem.at[h, 0, core, e], partner)

    n1 = 256
    n2 = 512

    def expert(e, carry):
        copies = weight_copies(e)
        copies[0].wait()
        copies[1].wait()

        def up(t, c2):
            rows = xo[e].reshape(chips * CORES * cap, d_model)
            cols = pl.ds(pl.multiple_of(t * n1, n1), n1)
            a = jnp.dot(rows, w1[e, :, cols], preferred_element_type=F32)
            b = jnp.dot(rows, w3[e, :, cols], preferred_element_type=F32)
            hid[:, cols] = (a * jax.nn.sigmoid(a) * b).astype(BF16)
            return c2

        lax.fori_loop(0, d_expert // n1, up, 0)
        copies[2].wait()

        def down(t, c2):
            cols = pl.ds(pl.multiple_of(t * n2, n2), n2)
            o = jnp.dot(hid[...], w2[e, :, cols], preferred_element_type=F32).astype(BF16)
            xo[e, :, :, :, cols] = o.reshape(side, side, CORES * cap, n2)
            return c2

        for h in range(2):
            lax.fori_loop(h * half // n2, (h + 1) * half // n2, down, 0)
            for k in near:
                for cm in range(CORES):
                    r1_copy(h, e, k, cm).start()
            r1_partner(h, e).start()
            cols = pl.ds(pl.multiple_of(h * half + core * quarter, quarter), quarter)
            mbuf[h, 0, core, e] = xo[e, my_y, :, :, cols] if h == 0 else xo[e, :, my_x, :, cols]
        return carry

    lax.fori_loop(0, local_experts, expert, 0)

    def r2_place(h, k):
        if h == 0:
            return my_y, ring(my_x, k)
        return ring(my_y, k), my_x

    def r2_copy(h, k, cd):
        y, x = r2_place(h, k)
        return remote(pbuf.at[h, k, cd], ybuf.at[h, k, core], r2_ssem.at[h, k, cd], r2_rsem.at[h, k, core], dev(y, x, cd))

    def r2_partner(h):
        return remote(pbuf.at[h, 0, 1 - core], ybuf.at[h, 0, core], r2_ssem.at[h, 0, 0], r2_rsem.at[h, 0, core], partner)

    def merge(h, k):
        y, x = r2_place(h, k)
        p = chip_at(y, x)
        q = x if h == 0 else y
        lhs = []
        for j in range(side):
            sy, sx = r1_place(h, side - j)
            base = pl.multiple_of(chip_at(sy, sx) * chip_experts, chip_experts)
            hit = slots[p, pl.ds(base, chip_experts), :][:, None, :] == wanted[None]
            g = gates[p, pl.ds(base, chip_experts), :]
            g_hi = g.astype(BF16).astype(F32)
            g_mid = (g - g_hi).astype(BF16).astype(F32)
            g_lo = g - g_hi - g_mid
            lhs.append(jnp.concatenate([
                jnp.where(hit, v[:, None, :], 0.0).reshape(chip_experts * CORES * cap, LANES).astype(BF16) for v in (g_hi, g_mid, g_lo)], axis=1))
        rows = mbuf[h, :, :, :, q].reshape(side * CORES * local_experts * CORES * cap, quarter)
        out = lax.dot_general(jnp.concatenate(lhs, axis=0), rows, (((0,), (0,)), ((), ())), preferred_element_type=F32)
        total = out[:LANES] + (out[LANES:2 * LANES] + out[2 * LANES:])
        pbuf[h, k] = total.reshape(CORES, num_tokens, quarter)

    def r1_arrived(h, k, c, e):
        pltpu.make_async_copy(mbuf.at[h, k, c, e], mbuf.at[h, k, c, e], r1_rsem.at[h, k, c, e]).wait()

    for h in range(2):
        def arrived(e, carry):
            for k in range(1, side):
                for c in range(CORES):
                    r1_arrived(h, k, c, e)
            r1_arrived(h, 0, 1 - core, e)
            return carry

        lax.fori_loop(0, local_experts, arrived, 0)

        def merge_remote(k, carry):
            merge(h, k)
            for cd in range(CORES):
                r2_copy(h, k, cd).start()
            return carry

        lax.fori_loop(1, side, merge_remote, 0)
        merge(h, 0)
        r2_partner(h).start()
        ybuf[h, 0, core] = pbuf[h, 0, core]

    for h in range(2):
        for k in near:
            for c in range(CORES):
                pltpu.make_async_copy(ybuf.at[h, k, c], ybuf.at[h, k, c], r2_rsem.at[h, k, c]).wait()
        pltpu.make_async_copy(ybuf.at[h, 0, 1 - core], ybuf.at[h, 0, 1 - core], r2_rsem.at[h, 0, 1 - core]).wait()
        for c in range(CORES):
            total = ybuf[h, 0, c]
            for k in range(1, side):
                total = total + ybuf[h, k, c]
            y_ref[:, pl.ds(h * half + c * quarter, quarter)] = total.astype(BF16)

    lax.fori_loop(1, num_devices, sent_meta, 0)

    def sent_blocks(a, carry):
        for h in range(2):
            for k in (1, side - 1):
                second_copy(h, a, k).wait_send()
            for b in range(side):
                core_copy(h, a, b).wait_send()
        return carry

    lax.fori_loop(0, side, sent_blocks, 0)
    for h in range(2):
        for k in range(1, side):
            first_copy(h, k).wait_send()
        for a in range(side):
            relay_copy(h, a, 1 if a < far else side - 1).wait_send()

    def sent_r1(e, carry):
        for h in range(2):
            for k in near:
                for cm in range(CORES):
                    r1_copy(h, e, k, cm).wait_send()
            r1_partner(h, e).wait_send()
        return carry

    lax.fori_loop(0, local_experts, sent_r1, 0)
    for h in range(2):
        for k in near:
            for cd in range(CORES):
                r2_copy(h, k, cd).wait_send()
        r2_partner(h).wait_send()


def solution(mesh):
    num_devices = mesh.shape['ep']
    side = math.isqrt(num_devices // CORES)
    row_spec = P(('dp', 'ep'), None)
    expert_spec = P('ep', None, None)

    def device_step(tokens, routes, w_router, w_one, w_three, w_two):
        num_tokens, d_model = tokens.shape
        top_k = routes.shape[1]
        num_experts = w_router.shape[1]
        local_experts, _, d_expert = w_one.shape
        cap = slot_capacity(num_tokens, top_k, num_experts)
        half = d_model // 2
        quarter = half // CORES
        chips = side * side
        any_spec = pl.BlockSpec(memory_space=pl.ANY)
        vmem_spec = pl.BlockSpec(memory_space=pltpu.VMEM)
        dma = pltpu.SemaphoreType.DMA
        return pl.pallas_call(
            functools.partial(moe_kernel, side),
            out_shape=jax.ShapeDtypeStruct((num_tokens, d_model), BF16),
            in_specs=[any_spec, vmem_spec, any_spec, any_spec, any_spec, any_spec],
            out_specs=vmem_spec,
            scratch_shapes=[
                pltpu.VMEM((2, num_devices, num_tokens, half), BF16),
                pltpu.VMEM((d_model, num_experts), BF16),
                pltpu.VMEM((local_experts, d_model, d_expert), BF16),
                pltpu.VMEM((local_experts, d_model, d_expert), BF16),
                pltpu.VMEM((local_experts, d_expert, d_model), BF16),
                pltpu.VMEM((local_experts, side, side, CORES * cap, d_model), BF16),
                pltpu.VMEM((chips * CORES * cap, d_expert), BF16),
                pltpu.VMEM((num_devices, 2 * top_k, LANES), F32),
                pltpu.VMEM((chips, num_experts, LANES), F32),
                pltpu.VMEM((chips, num_experts, LANES), F32),
                pltpu.VMEM((2, side, CORES, local_experts, side, CORES * cap, quarter), BF16),
                pltpu.VMEM((2, side, CORES, num_tokens, quarter), F32),
                pltpu.VMEM((2, side, CORES, num_tokens, quarter), F32),
                dma((2,)), dma((1,)), dma((3, local_experts)),
                dma((num_devices,)), dma((num_devices,)),
                dma((2, side)), dma((2, side, side)), dma((2, side)), dma((2, side, side)), dma((2, num_devices)),
                dma((2, side, CORES, local_experts)), dma((2, side, CORES, local_experts)),
                dma((2, side, CORES)), dma((2, side, CORES)),
            ],
            compiler_params=pltpu.CompilerParams(collective_id=0, has_side_effects=True, vmem_limit_bytes=67043328),
        )(tokens, routes.T, w_router, w_one, w_three, w_two)

    return jax.shard_map(device_step, mesh=mesh, in_specs=(row_spec, row_spec, P(None, None), expert_spec, expert_spec, expert_spec), out_specs=row_spec, check_vma=False)
```

```python
import functools
import math

import jax
import jax.numpy as jnp
from jax import lax
from jax.experimental import pallas as pl
from jax.experimental.pallas import tpu as pltpu
from jax.sharding import PartitionSpec as P

MESH = pl.DeviceIdType.MESH
F32 = jnp.float32
BF16 = jnp.bfloat16
CORES = 2
LANES = 128


def slot_capacity(num_tokens, top_k, num_experts):
    return 8 * ((3 * num_tokens * top_k + 16 * num_experts - 1) // (16 * num_experts))


def moe_kernel(
    side,
    x_hbm, routes_ref, wr_hbm, w1_hbm, w3_hbm, w2_hbm, y_ref,
    xg, wr, w13, w2, xo, hid, meta, slots, gates, mbuf, pbuf, ybuf,
    x_sem, wr_sem, w_sem, meta_ssem, meta_rsem, ag_ssem, ag_rsem, core_rsem,
    r1_ssem, r1_rsem, r2_ssem, r2_rsem,
):
    num_devices = CORES * side * side
    chips = side * side
    num_tokens, d_model = x_hbm.shape
    half = d_model // 2
    quarter = half // CORES
    local_experts, _, _, d_expert = w13.shape
    chip_experts = CORES * local_experts
    num_experts = num_devices * local_experts
    top_k = routes_ref.shape[0]
    cap = xo.shape[3] // CORES

    me = lax.axis_index('ep')
    core = lax.rem(me, CORES)
    my_x = lax.rem(lax.div(me, CORES), side)
    my_y = lax.div(me, CORES * side)

    def ring(v, k):
        return lax.rem(v + k, side)

    def chip_at(y, x):
        return y * side + x

    def dev(y, x, c):
        return chip_at(y, x) * CORES + c

    partner = dev(my_y, my_x, 1 - core)

    def remote(src, dst, ssem, rsem, target):
        return pltpu.make_async_remote_copy(src_ref=src, dst_ref=dst, send_sem=ssem, recv_sem=rsem, device_id={'ep': target}, device_id_type=MESH)

    barrier = pltpu.get_barrier_semaphore()

    def greet(i, carry):
        pl.semaphore_signal(barrier, inc=1, device_id={'ep': lax.rem(me + i, num_devices)}, device_id_type=MESH)
        return carry

    lax.fori_loop(1, num_devices, greet, 0)

    x_copies = [pltpu.make_async_copy(x_hbm.at[:, pl.ds(h * half, half)], xg.at[h, me], x_sem) for h in range(2)]
    for cp in x_copies:
        cp.start()
    wr_copy = pltpu.make_async_copy(wr_hbm, wr, wr_sem)
    wr_copy.start()

    def weight_copies(e):
        return [
            pltpu.make_async_copy(w1_hbm.at[e], w13.at[e, 0], w_sem.at[0, e]),
            pltpu.make_async_copy(w3_hbm.at[e], w13.at[e, 1], w_sem.at[0, e]),
            pltpu.make_async_copy(w2_hbm.at[e], w2.at[e], w_sem.at[1, e]),
        ]

    def start_weights(e, carry):
        for cp in weight_copies(e):
            cp.start()
        return carry

    lax.fori_loop(0, local_experts, start_weights, 0)


    pltpu.make_async_copy(xg.at[:, me], xg.at[:, me], x_sem).wait()

    wr_copy.wait()
    x_local = [xg[h, me] for h in range(2)]
    logits = sum(
        lax.dot_general(wr[pl.ds(h * half, half), :], x_local[h], (((0,), (1,)), ((), ())), preferred_element_type=F32)
        for h in range(2)
    )
    routes = routes_ref[...]
    expert_iota = lax.broadcasted_iota(jnp.int32, (num_experts, num_tokens), 0)
    picked = jnp.concatenate(
        [jnp.sum(jnp.where(expert_iota == routes[j:j + 1, :], logits, 0.0), axis=0, keepdims=True) for j in range(top_k)], axis=0)
    ex = jnp.exp(picked - jnp.max(picked, axis=0, keepdims=True))
    gate = ex / jnp.sum(ex, axis=0, keepdims=True)
    meta[me] = jnp.concatenate([routes.astype(F32) + 1.0, gate], axis=1)

    pl.semaphore_wait(barrier, num_devices - 1)

    def place(h, a, b):
        if h == 0:
            return ring(my_y, b), ring(my_x, a)
        return ring(my_y, a), ring(my_x, b)

    def block_src(h, a, b, c):
        y, x = place(h, a, b)
        return dev(y, x, c)

    def move_block(h, src, rsem, target):
        return remote(xg.at[h, src], xg.at[h, src], ag_ssem.at[h], rsem, target)

    def first_copy(h, k):
        return move_block(h, me, ag_rsem.at[side - k, 0], block_src(h, k, 0, core))

    def second_copy(h, a, k):
        return move_block(h, block_src(h, a, 0, core), ag_rsem.at[a, side - k], block_src(h, 0, k, core))

    def relay_copy(h, a, k):
        return move_block(h, block_src(h, a, k, core), ag_rsem.at[a, side // 2], block_src(h, 0, side - k, core))

    def core_copy(h, a, b):
        return move_block(h, block_src(h, a, b, core), core_rsem.at[a, b], partner)

    def wait_blocks(sem):
        pltpu.make_async_copy(xg.at[:, me], xg.at[:, me], sem).wait()

    def meta_copy(i):
        return remote(meta.at[me], meta.at[me], meta_ssem, meta_rsem, lax.rem(me + i, num_devices))

    def send_meta(i, carry):
        meta_copy(i).start()
        return carry

    def wait_meta(sem):
        others = meta.at[pl.ds(0, num_devices - 1)]
        pltpu.make_async_copy(others, others, sem).wait()

    lax.fori_loop(1, num_devices, send_meta, 0)
    for h in range(2):
        for k in (1, side - 1) + tuple(range(2, side - 1)):
            first_copy(h, k).start()
        for k in (1, side - 1):
            second_copy(h, 0, k).start()
        core_copy(h, 0, 0).start()

    row_i = lax.broadcasted_iota(jnp.int32, (LANES, LANES), 0)
    col_i = lax.broadcasted_iota(jnp.int32, (LANES, LANES), 1)
    before = jnp.where((row_i < col_i) & (row_i // num_tokens == col_i // num_tokens), 1.0, 0.0).astype(BF16)
    ids = lax.broadcasted_iota(jnp.int32, (num_experts, LANES), 0).astype(F32) + 1.0

    def plan_chip(p, carry):
        tiles = [meta[CORES * p + c] for c in range(CORES)]
        turned = [pltpu.roll(v, num_tokens, 1) for v in tiles]
        low = lax.broadcasted_iota(jnp.int32, tiles[0].shape, 1) < num_tokens
        picks = jnp.where(low, tiles[0], turned[1])
        shares = jnp.where(low, turned[0], tiles[1])
        mask = jnp.zeros((num_experts, LANES), F32)
        weight = jnp.zeros((num_experts, LANES), F32)
        for j in range(top_k):
            hit = ids == picks[j:j + 1, :]
            mask = jnp.where(hit, 1.0, mask)
            weight = jnp.where(hit, shares[j:j + 1, :], weight)
        rank = jnp.dot(mask.astype(BF16), before, preferred_element_type=F32)
        slots[p] = jnp.where(mask > 0.0, rank, -1.0)
        gates[p] = weight
        return carry


    pair_row = lax.broadcasted_iota(jnp.int32, (CORES * cap, LANES), 0)
    pair_lane = lax.broadcasted_iota(jnp.int32, (CORES * cap, LANES), 1)
    wanted = jnp.where(pair_row // cap == pair_lane // num_tokens, pair_row % cap, -2).astype(F32)

    def gather_chip(h, y, x):
        p = chip_at(y, x)
        mine = slots[p, pl.ds(me * local_experts, local_experts), :]
        pick = jnp.where(mine[:, None, :] == wanted[None], 1.0, 0.0).reshape(local_experts * CORES * cap, LANES).astype(BF16)
        rows = xg[h, pl.ds(p * CORES, CORES)].reshape(CORES * num_tokens, half)
        out = jnp.dot(pick, rows, preferred_element_type=F32).astype(BF16)
        xo[:, y, x, :, pl.ds(h * half, half)] = out.reshape(local_experts, CORES * cap, half)

    def finish(a, b):
        wait_blocks(core_rsem.at[a, b])
        for h in range(2):
            gather_chip(h, *place(h, a, b))

    def land(a, b):
        wait_blocks(ag_rsem.at[a, b])
        for h in range(2):
            core_copy(h, a, b).start()

    far = side // 2
    near = (1, side - 1) + tuple(range(2, side - 1))

    def same_line(a):
        land(a, 0)
        for h in range(2):
            for k in (1, side - 1):
                second_copy(h, a, k).start()

    def next_lines(a, carry):
        land(a, 1)
        for h in range(2):
            relay_copy(h, a, 1).start()
        land(a + far, side - 1)
        for h in range(2):
            relay_copy(h, a + far, side - 1).start()
        land(a + far, 1)
        land(a, side - 1)
        finish(a, 0)
        finish(a + far, 0)
        return carry

    def far_line(a, carry):
        land(a, far)
        finish(a, 1)
        finish(a, side - 1)
        return carry

    def far_lines(a, carry):
        far_line(a, carry)
        finish(a - 1, far)
        return carry

    for a in near:
        same_line(a)
    wait_meta(meta_rsem)
    lax.fori_loop(0, chips, plan_chip, 0)
    lax.fori_loop(0, far, next_lines, 0)
    far_line(0, 0)
    lax.fori_loop(1, side, far_lines, 0)
    finish(side - 1, far)

    def r1_place(h, k):
        if h == 0:
            return ring(my_y, k), my_x
        return my_y, ring(my_x, k)

    def r1_src(h, e, k, cm):
        y, x = r1_place(h, k)
        cols = pl.ds(h * half + cm * quarter, quarter)
        if h == 0:
            return xo.at[e, y, :, :, cols]
        return xo.at[e, :, x, :, cols]

    def r1_copy(h, e, k, cm):
        y, x = r1_place(h, k)
        return remote(r1_src(h, e, k, cm), mbuf.at[h, k, core, e], r1_ssem.at[0], r1_rsem.at[h, k], dev(y, x, cm))

    def r1_partner(h, e):
        y, x = my_y, my_x
        cols = pl.ds(pl.multiple_of(h * half + (1 - core) * quarter, quarter), quarter)
        src = xo.at[e, y, :, :, cols] if h == 0 else xo.at[e, :, x, :, cols]
        return remote(src, mbuf.at[h, 0, core, e], r1_ssem.at[1], r1_rsem.at[h, 0], partner)

    n1 = 256
    n2 = 512

    def expert(e, carry):
        pltpu.make_async_copy(w13.at[e], w13.at[e], w_sem.at[0, e]).wait()

        def up(t, c2):
            rows = xo[e].reshape(chips * CORES * cap, d_model)
            cols = pl.ds(pl.multiple_of(t * n1, n1), n1)
            a = jnp.dot(rows, w13[e, 0, :, cols], preferred_element_type=F32)
            b = jnp.dot(rows, w13[e, 1, :, cols], preferred_element_type=F32)
            hid[:, cols] = (a * jax.nn.sigmoid(a) * b).astype(BF16)
            return c2

        lax.fori_loop(0, d_expert // n1, up, 0)
        weight_copies(e)[2].wait()

        def down(t, c2):
            cols = pl.ds(pl.multiple_of(t * n2, n2), n2)
            o = jnp.dot(hid[...], w2[e, :, cols], preferred_element_type=F32).astype(BF16)
            xo[e, :, :, :, cols] = o.reshape(side, side, CORES * cap, n2)
            return c2

        for h in range(2):
            lax.fori_loop(h * half // n2, (h + 1) * half // n2, down, 0)
            for k in near:
                for cm in range(CORES):
                    r1_copy(h, e, k, cm).start()
            r1_partner(h, e).start()
            cols = pl.ds(pl.multiple_of(h * half + core * quarter, quarter), quarter)
            mbuf[h, 0, core, e] = xo[e, my_y, :, :, cols] if h == 0 else xo[e, :, my_x, :, cols]
        return carry

    lax.fori_loop(0, local_experts, expert, 0)

    def r2_place(h, k):
        if h == 0:
            return my_y, ring(my_x, k)
        return ring(my_y, k), my_x

    def r2_copy(h, k, cd):
        y, x = r2_place(h, k)
        return remote(pbuf.at[h, k, cd], ybuf.at[h, k, core], r2_ssem.at[0], r2_rsem.at[h, 0], dev(y, x, cd))

    def r2_partner(h):
        return remote(pbuf.at[h, 0, 1 - core], ybuf.at[h, 0, core], r2_ssem.at[1], r2_rsem.at[h, 1], partner)

    def merge(h, k):
        y, x = r2_place(h, k)
        p = chip_at(y, x)
        q = x if h == 0 else y
        lhs = []
        for j in range(side):
            sy, sx = r1_place(h, side - j)
            base = pl.multiple_of(chip_at(sy, sx) * chip_experts, chip_experts)
            hit = slots[p, pl.ds(base, chip_experts), :][:, None, :] == wanted[None]
            g = gates[p, pl.ds(base, chip_experts), :]
            g_hi = g.astype(BF16).astype(F32)
            g_mid = (g - g_hi).astype(BF16).astype(F32)
            g_lo = g - g_hi - g_mid
            lhs.append(jnp.concatenate([
                jnp.where(hit, v[:, None, :], 0.0).reshape(chip_experts * CORES * cap, LANES).astype(BF16) for v in (g_hi, g_mid, g_lo)], axis=1))
        rows = mbuf[h, :, :, :, q].reshape(side * CORES * local_experts * CORES * cap, quarter)
        out = lax.dot_general(jnp.concatenate(lhs, axis=0), rows, (((0,), (0,)), ((), ())), preferred_element_type=F32)
        total = out[:LANES] + (out[LANES:2 * LANES] + out[2 * LANES:])
        pbuf[h, k] = total.reshape(CORES, num_tokens, quarter)

    def wait_bytes(ref, sem):
        pltpu.make_async_copy(ref, ref, sem).wait()

    for h in range(2):
        for k in range(1, side):
            wait_bytes(mbuf.at[h, k], r1_rsem.at[h, k])
        wait_bytes(mbuf.at[h, 0, 1 - core], r1_rsem.at[h, 0])

    def merge_remote(i, carry):
        k = lax.rem(i + 1, side - 1) + 1
        for h in range(2):
            merge(h, k)
            for cd in range(CORES):
                r2_copy(h, k, cd).start()
        return carry

    lax.fori_loop(0, side - 1, merge_remote, 0)
    for h in range(2):
        merge(h, 0)
        r2_partner(h).start()
        ybuf[h, 0, core] = pbuf[h, 0, core]

    for h in range(2):
        wait_bytes(ybuf.at[h, pl.ds(1, side - 1)], r2_rsem.at[h, 0])
        wait_bytes(ybuf.at[h, 0, 1 - core], r2_rsem.at[h, 1])
        for c in range(CORES):
            total = ybuf[h, 0, c]
            for k in range(1, side):
                total = total + ybuf[h, k, c]
            y_ref[:, pl.ds(h * half + c * quarter, quarter)] = total.astype(BF16)

    wait_meta(meta_ssem)
    for h in range(2):
        wait_bytes(xg.at[h, pl.ds(0, side - 1 + 2 * side + side + chips)], ag_ssem.at[h])
    wait_bytes(mbuf.at[:, pl.ds(1, side - 1)], r1_ssem.at[0])
    wait_bytes(mbuf.at[:, 0, 0], r1_ssem.at[1])
    wait_bytes(pbuf.at[:, pl.ds(1, side - 1)], r2_ssem.at[0])
    wait_bytes(pbuf.at[:, 0, 0], r2_ssem.at[1])


def solution(mesh):
    num_devices = mesh.shape['ep']
    side = math.isqrt(num_devices // CORES)
    row_spec = P(('dp', 'ep'), None)
    expert_spec = P('ep', None, None)

    def device_step(tokens, routes, w_router, w_one, w_three, w_two):
        num_tokens, d_model = tokens.shape
        top_k = routes.shape[1]
        num_experts = w_router.shape[1]
        local_experts, _, d_expert = w_one.shape
        cap = slot_capacity(num_tokens, top_k, num_experts)
        half = d_model // 2
        quarter = half // CORES
        chips = side * side
        any_spec = pl.BlockSpec(memory_space=pl.ANY)
        vmem_spec = pl.BlockSpec(memory_space=pltpu.VMEM)
        dma = pltpu.SemaphoreType.DMA
        return pl.pallas_call(
            functools.partial(moe_kernel, side),
            out_shape=jax.ShapeDtypeStruct((num_tokens, d_model), BF16),
            in_specs=[any_spec, vmem_spec, any_spec, any_spec, any_spec, any_spec],
            out_specs=vmem_spec,
            scratch_shapes=[
                pltpu.VMEM((2, num_devices, num_tokens, half), BF16),
                pltpu.VMEM((d_model, num_experts), BF16),
                pltpu.VMEM((local_experts, 2, d_model, d_expert), BF16),
                pltpu.VMEM((local_experts, d_expert, d_model), BF16),
                pltpu.VMEM((local_experts, side, side, CORES * cap, d_model), BF16),
                pltpu.VMEM((chips * CORES * cap, d_expert), BF16),
                pltpu.VMEM((num_devices, top_k, LANES), F32),
                pltpu.VMEM((chips, num_experts, LANES), F32),
                pltpu.VMEM((chips, num_experts, LANES), F32),
                pltpu.VMEM((2, side, CORES, local_experts, side, CORES * cap, quarter), BF16),
                pltpu.VMEM((2, side, CORES, num_tokens, quarter), F32),
                pltpu.VMEM((2, side, CORES, num_tokens, quarter), F32),
                dma, dma, dma((2, local_experts)), dma, dma, dma((2,)), dma((side, side)), dma((side, side)),
                dma((2,)), dma((2, side)), dma((2,)), dma((2, 2)),
            ],
            compiler_params=pltpu.CompilerParams(collective_id=0, has_side_effects=True, vmem_limit_bytes=67043328),
        )(tokens, routes.T, w_router, w_one, w_three, w_two)

    return jax.shard_map(device_step, mesh=mesh, in_specs=(row_spec, row_spec, P(None, None), expert_spec, expert_spec, expert_spec), out_specs=row_spec, check_vma=False)
```

```python
import functools
import math

import jax
import jax.numpy as jnp
from jax import lax
from jax.experimental import pallas as pl
from jax.experimental.pallas import tpu as pltpu
from jax.sharding import PartitionSpec as P

MESH = pl.DeviceIdType.MESH
F32 = jnp.float32
BF16 = jnp.bfloat16
CORES = 2
LANES = 128


def slot_capacity(num_tokens, top_k, num_experts):
    return 8 * ((3 * num_tokens * top_k + 16 * num_experts - 1) // (16 * num_experts))


def moe_kernel(
    side,
    x_hbm, routes_hbm, wr_hbm, w1_hbm, w3_hbm, w2_hbm, y_ref,
    xg, routes_ref, wr, w13, w2, xo, hid, meta, slots, gates, mbuf, pbuf, ybuf,
    x_sem, wr_sem, routes_sem, w_sem, meta_ssem, meta_rsem, ag_ssem, ag_rsem, core_rsem,
    r1_ssem, r1_rsem, r2_ssem, r2_rsem,
):
    num_devices = CORES * side * side
    chips = side * side
    num_tokens, d_model = x_hbm.shape
    half = d_model // 2
    quarter = half // CORES
    piece = quarter // 2
    local_experts, _, _, d_expert = w13.shape
    chip_experts = CORES * local_experts
    num_experts = num_devices * local_experts
    top_k = routes_ref.shape[0]
    cap = xo.shape[3] // CORES

    me = lax.axis_index('ep')
    core = lax.rem(me, CORES)
    my_x = lax.rem(lax.div(me, CORES), side)
    my_y = lax.div(me, CORES * side)

    def ring(v, k):
        return lax.rem(v + k, side)

    far = side // 2

    def spot(k):
        return k + (k // far) * (side + 1 - 2 * k)

    def chip_at(y, x):
        return y * side + x

    def dev(y, x, c):
        return chip_at(y, x) * CORES + c

    partner = dev(my_y, my_x, 1 - core)

    def remote(src, dst, ssem, rsem, target):
        return pltpu.make_async_remote_copy(src_ref=src, dst_ref=dst, send_sem=ssem, recv_sem=rsem, device_id={'ep': target}, device_id_type=MESH)

    barrier = pltpu.get_barrier_semaphore()

    def greet(i, carry):
        pl.semaphore_signal(barrier, inc=1, device_id={'ep': lax.rem(me + i, num_devices)}, device_id_type=MESH)
        return carry

    lax.fori_loop(1, num_devices, greet, 0)

    x_copies = [pltpu.make_async_copy(x_hbm.at[:, pl.ds(h * half, half)], xg.at[h, me], x_sem) for h in range(2)]
    for cp in x_copies:
        cp.start()
    wr_copy = pltpu.make_async_copy(wr_hbm, wr, wr_sem)
    wr_copy.start()
    routes_copy = pltpu.make_async_copy(routes_hbm, routes_ref, routes_sem)
    routes_copy.start()

    def weight_copies(e):
        return [
            pltpu.make_async_copy(w1_hbm.at[e], w13.at[e, 0], w_sem.at[0, e]),
            pltpu.make_async_copy(w3_hbm.at[e], w13.at[e, 1], w_sem.at[0, e]),
            pltpu.make_async_copy(w2_hbm.at[e], w2.at[e], w_sem.at[1, e]),
        ]

    def start_weights(e, carry):
        for cp in weight_copies(e):
            cp.start()
        return carry

    lax.fori_loop(0, local_experts, start_weights, 0)


    pltpu.make_async_copy(xg.at[:, me], xg.at[:, me], x_sem).wait()

    wr_copy.wait()
    routes_copy.wait()
    x_local = [xg[h, me] for h in range(2)]
    logits = sum(
        lax.dot_general(wr[pl.ds(h * half, half), :], x_local[h], (((0,), (1,)), ((), ())), preferred_element_type=F32)
        for h in range(2)
    )
    routes = routes_ref[...]
    expert_iota = lax.broadcasted_iota(jnp.int32, (num_experts, num_tokens), 0)
    picked = jnp.concatenate(
        [jnp.sum(jnp.where(expert_iota == routes[j:j + 1, :], logits, 0.0), axis=0, keepdims=True) for j in range(top_k)], axis=0)
    ex = jnp.exp(picked - jnp.max(picked, axis=0, keepdims=True))
    gate = ex / jnp.sum(ex, axis=0, keepdims=True)
    meta[me] = jnp.concatenate([routes.astype(F32) + 1.0, gate], axis=1)

    pl.semaphore_wait(barrier, num_devices - 1)

    def place(h, a, b):
        if h == 0:
            return ring(my_y, b), ring(my_x, a)
        return ring(my_y, a), ring(my_x, b)

    def block_src(h, a, b, c):
        y, x = place(h, a, b)
        return dev(y, x, c)

    def move_block(h, src, rsem, target):
        return remote(xg.at[h, src], xg.at[h, src], ag_ssem.at[h], rsem, target)

    def first_copy(h, k):
        return move_block(h, me, ag_rsem.at[side - k, 0], block_src(h, k, 0, core))

    def first_relay(h):
        k = 1 + core * (side - 2)
        return move_block(h, block_src(h, k, 0, core), ag_rsem.at[side // 2, 0], block_src(h, side - k, 0, core))

    def second_copy(h, a, k):
        return move_block(h, block_src(h, a, 0, core), ag_rsem.at[a, side - k], block_src(h, 0, k, core))

    def relay_copy(h, a, k):
        return move_block(h, block_src(h, a, k, core), ag_rsem.at[a, side // 2], block_src(h, 0, side - k, core))

    def core_copy(h, a, b):
        return move_block(h, block_src(h, a, b, core), core_rsem.at[a, b], partner)

    def wait_blocks(sem):
        pltpu.make_async_copy(xg.at[:, me], xg.at[:, me], sem).wait()

    def meta_copy(i):
        return remote(meta.at[me], meta.at[me], meta_ssem, meta_rsem, lax.rem(me + i, num_devices))

    def send_meta(i, carry):
        meta_copy(i).start()
        return carry

    def wait_meta(sem):
        others = meta.at[pl.ds(0, num_devices - 1)]
        pltpu.make_async_copy(others, others, sem).wait()

    for h in range(2):
        for k in (1, side - 1):
            first_copy(h, k).start()
    lax.fori_loop(1, num_devices, send_meta, 0)
    for h in range(2):
        for k in (1, side - 1):
            second_copy(h, 0, k).start()
        core_copy(h, 0, 0).start()

    row_i = lax.broadcasted_iota(jnp.int32, (LANES, LANES), 0)
    col_i = lax.broadcasted_iota(jnp.int32, (LANES, LANES), 1)
    before = jnp.where((row_i < col_i) & (row_i // num_tokens == col_i // num_tokens), 1.0, 0.0).astype(BF16)
    ids = lax.broadcasted_iota(jnp.int32, (num_experts, LANES), 0).astype(F32) + 1.0

    def plan_chip(p, carry):
        tiles = [meta[CORES * p + c] for c in range(CORES)]
        turned = [pltpu.roll(v, num_tokens, 1) for v in tiles]
        low = lax.broadcasted_iota(jnp.int32, tiles[0].shape, 1) < num_tokens
        picks = jnp.where(low, tiles[0], turned[1])
        shares = jnp.where(low, turned[0], tiles[1])
        mask = jnp.zeros((num_experts, LANES), F32)
        weight = jnp.zeros((num_experts, LANES), F32)
        for j in range(top_k):
            hit = ids == picks[j:j + 1, :]
            mask = jnp.where(hit, 1.0, mask)
            weight = jnp.where(hit, shares[j:j + 1, :], weight)
        rank = jnp.dot(mask.astype(BF16), before, preferred_element_type=F32)
        slots[p] = jnp.where(mask > 0.0, rank, -1.0)
        gates[p] = weight
        return carry


    pair_row = lax.broadcasted_iota(jnp.int32, (CORES * cap, LANES), 0)
    pair_lane = lax.broadcasted_iota(jnp.int32, (CORES * cap, LANES), 1)
    wanted = jnp.where(pair_row // cap == pair_lane // num_tokens, pair_row % cap, -2).astype(F32)

    def gather_chip(h, a, b):
        p = chip_at(*place(h, a, b))
        py, px = (spot(b), spot(a)) if h == 0 else (spot(a), spot(b))
        mine = slots[p, pl.ds(me * local_experts, local_experts), :]
        pick = jnp.where(mine[:, None, :] == wanted[None], 1.0, 0.0).reshape(local_experts * CORES * cap, LANES).astype(BF16)
        rows = xg[h, pl.ds(p * CORES, CORES)].reshape(CORES * num_tokens, half)
        out = jnp.dot(pick, rows, preferred_element_type=F32).astype(BF16)
        xo[:, py, px, :, pl.ds(h * half, half)] = out.reshape(local_experts, CORES * cap, half)

    def finish(a, b):
        wait_blocks(core_rsem.at[a, b])
        for h in range(2):
            gather_chip(h, a, b)

    def land(a, b):
        wait_blocks(ag_rsem.at[a, b])
        for h in range(2):
            core_copy(h, a, b).start()

    near = (1, side - 1) + tuple(range(2, side - 1))

    def same_line(a):
        for h in range(2):
            for k in (1, side - 1):
                second_copy(h, a, k).start()

    def next_lines(a, carry):
        land(a, 1)
        for h in range(2):
            relay_copy(h, a, 1).start()
        land(a + far, side - 1)
        for h in range(2):
            relay_copy(h, a + far, side - 1).start()
        land(a + far, 1)
        land(a, side - 1)
        finish(a, 0)
        finish(a + far, 0)
        return carry

    def near_lines(p, carry):
        finish(spot(p), 1)
        finish(spot(p), side - 1)
        return carry

    def far_lines(p, carry):
        finish(spot(p), far)
        return carry

    for a in near[:2]:
        land(a, 0)
    for h in range(2):
        first_relay(h).start()
    for a in near[:2]:
        same_line(a)
    wait_meta(meta_rsem)
    lax.fori_loop(0, chips, plan_chip, 0)
    land(far, 0)
    same_line(far)
    lax.fori_loop(0, far, next_lines, 0)
    lax.fori_loop(0, side - 1, near_lines, 0)

    def r1_place(h, k):
        if h == 0:
            return ring(my_y, k), my_x
        return my_y, ring(my_x, k)

    close, edge = pl.ds(0, side - 1), pl.ds(side - 1, 1)
    whole = pl.ds(0, side)
    n_close = (side - 1) * (side - 1) * CORES * cap
    n_rows = chips * CORES * cap
    lines = {
        'near': [(0, close)] + [(k, close) for k in (1, side - 1)],
        'far': [(0, edge)] + [(far, whole)] + [(k, edge) for k in (1, side - 1)],
        'all': [(0, whole)] + [(k, whole) for k in (far, 1, side - 1)],
    }
    spans = {'near': pl.ds(0, n_close), 'far': pl.ds(n_close, n_rows - n_close), 'all': pl.ds(0, n_rows)}

    def read_rows(part, e):
        if part == 'near':
            return xo[e, close, close].reshape(n_close, d_model)
        if part == 'far':
            n_edge = side * CORES * cap
            return jnp.concatenate([xo[e, side - 1].reshape(n_edge, d_model), xo[e, close, side - 1].reshape(n_rows - n_close - n_edge, d_model)], axis=0)
        return xo[e].reshape(n_rows, d_model)

    def write_rows(part, e, cols, o):
        n = o.shape[1]
        if part == 'near':
            xo[e, close, close, :, cols] = o.reshape(side - 1, side - 1, CORES * cap, n)
        elif part == 'far':
            n_edge = side * CORES * cap
            xo[e, side - 1, :, :, cols] = o[:n_edge].reshape(side, CORES * cap, n)
            xo[e, close, side - 1, :, cols] = o[n_edge:].reshape(side - 1, CORES * cap, n)
        else:
            xo[e, :, :, :, cols] = o.reshape(side, side, CORES * cap, n)

    def line_ref(h, e, k, span, cols):
        return xo.at[e, spot(k), span, :, cols] if h == 0 else xo.at[e, span, spot(k), :, cols]

    def cols_of(g, h, c):
        return pl.ds(pl.multiple_of(h * half + c * quarter + g * piece, piece), piece)

    def r1_copy(g, h, e, k, span, cm):
        y, x = r1_place(h, k)
        src = line_ref(h, e, k, span, cols_of(g, h, cm))
        return remote(src, mbuf.at[g, h, k, core, e, span], r1_ssem.at[0], r1_rsem.at[g, h, k], dev(y, x, cm))

    def r1_partner(g, h, e, span):
        src = line_ref(h, e, 0, span, cols_of(g, h, 1 - core))
        return remote(src, mbuf.at[g, h, 0, core, e, span], r1_ssem.at[1], r1_rsem.at[g, h, 0], partner)

    n1 = 256

    def up_rows(part, e):
        if part != 'far':
            pltpu.make_async_copy(w13.at[e], w13.at[e], w_sem.at[0, e]).wait()

        def up(t, carry):
            rows = read_rows(part, e)
            cols = pl.ds(pl.multiple_of(t * n1, n1), n1)
            a = jnp.dot(rows, w13[e, 0, :, cols], preferred_element_type=F32)
            b = jnp.dot(rows, w13[e, 1, :, cols], preferred_element_type=F32)
            hid[e % 2, spans[part], cols] = (a * jax.nn.sigmoid(a) * b).astype(BF16)
            return carry

        lax.fori_loop(0, d_expert // n1, up, 0)

    def send_rows(part, e, g, h):
        for k, span in lines[part][1:]:
            for cm in range(CORES):
                r1_copy(g, h, e, k, span, cm).start()
        span = lines[part][0][1]
        r1_partner(g, h, e, span).start()
        cols = cols_of(g, h, core)
        mbuf[g, h, 0, core, e, span] = xo[e, 0, span, :, cols] if h == 0 else xo[e, span, 0, :, cols]

    def down_group(part, e, g):
        for h in range(2):
            def down(c, carry):
                cols = cols_of(g, h, c)
                write_rows(part, e, cols, jnp.dot(hid[e % 2, spans[part], :], w2[e, :, cols], preferred_element_type=F32).astype(BF16))
                return carry

            lax.fori_loop(0, CORES, down, 0)
            send_rows(part, e, g, h)

    def wait_down(e):
        pltpu.make_async_copy(w2.at[e], w2.at[e], w_sem.at[1, e]).wait()

    def down_rows(part, e):
        if part != 'far':
            wait_down(e)

        def down(t, carry):
            cols = pl.ds(pl.multiple_of(t * quarter, quarter), quarter)
            write_rows(part, e, cols, jnp.dot(hid[e % 2, spans[part], :], w2[e, :, cols], preferred_element_type=F32).astype(BF16))
            return carry

        for h in range(2):
            lax.fori_loop(h * CORES, (h + 1) * CORES, down, 0)
            for g in range(2):
                send_rows(part, e, g, h)

    early = 2

    def near_expert(e, carry):
        up_rows('near', e)
        for i in range(far):
            land(spot(e * far + i), far)
        down_rows('near', e)
        return carry

    def far_expert(e, carry):
        up_rows('far', e)
        down_rows('far', e)
        return carry

    def all_expert(e, carry):
        up_rows('all', e)
        wait_down(e)
        down_group('all', e, 0)
        return carry

    def all_second(e, carry):
        down_group('all', e, 1)
        return carry

    lax.fori_loop(0, early, near_expert, 0)
    finish(far, 1)
    finish(far, side - 1)
    lax.fori_loop(0, side, far_lines, 0)
    lax.fori_loop(0, early, far_expert, 0)
    lax.fori_loop(early, local_experts, all_expert, 0)
    lax.fori_loop(early, local_experts, all_second, 0)

    def r2_place(h, k):
        if h == 0:
            return my_y, ring(my_x, k)
        return ring(my_y, k), my_x

    def r2_copy(g, h, k, cd):
        y, x = r2_place(h, k)
        return remote(pbuf.at[g, h, k, cd], ybuf.at[g, h, k, core], r2_ssem.at[0], r2_rsem.at[g, h, 0], dev(y, x, cd))

    def r2_partner(g, h):
        return remote(pbuf.at[g, h, 0, 1 - core], ybuf.at[g, h, 0, core], r2_ssem.at[1], r2_rsem.at[g, h, 1], partner)

    def merge(g, h, k):
        y, x = r2_place(h, k)
        p = chip_at(y, x)
        q = spot(k)
        lhs = []
        for j in range(side):
            sy, sx = r1_place(h, side - j)
            base = pl.multiple_of(chip_at(sy, sx) * chip_experts, chip_experts)
            hit = slots[p, pl.ds(base, chip_experts), :][:, None, :] == wanted[None]
            share = gates[p, pl.ds(base, chip_experts), :]
            g_hi = share.astype(BF16).astype(F32)
            g_mid = (share - g_hi).astype(BF16).astype(F32)
            g_lo = share - g_hi - g_mid
            lhs.append(jnp.concatenate([
                jnp.where(hit, v[:, None, :], 0.0).reshape(chip_experts * CORES * cap, LANES).astype(BF16) for v in (g_hi, g_mid, g_lo)], axis=1))
        rows = mbuf[g, h, :, :, :, q].reshape(side * CORES * local_experts * CORES * cap, piece)
        out = lax.dot_general(jnp.concatenate(lhs, axis=0), rows, (((0,), (0,)), ((), ())), preferred_element_type=F32)
        total = out[:LANES] + (out[LANES:2 * LANES] + out[2 * LANES:])
        pbuf[g, h, k] = total.reshape(CORES, num_tokens, piece)

    def wait_bytes(ref, sem):
        pltpu.make_async_copy(ref, ref, sem).wait()

    def merge_group(g, carry):
        for h in range(2):
            for k in range(1, side):
                wait_bytes(mbuf.at[g, h, k], r1_rsem.at[g, h, k])
            wait_bytes(mbuf.at[g, h, 0, 1 - core], r1_rsem.at[g, h, 0])

        def merge_remote(i, c2):
            k = lax.rem(i + 1, side - 1) + 1
            for h in range(2):
                merge(g, h, k)
                for cd in range(CORES):
                    r2_copy(g, h, k, cd).start()
            return c2

        lax.fori_loop(0, side - 1, merge_remote, 0)
        for h in range(2):
            merge(g, h, 0)
            r2_partner(g, h).start()
            ybuf[g, h, 0, core] = pbuf[g, h, 0, core]
        return carry

    lax.fori_loop(0, 2, merge_group, 0)

    for g in range(2):
        for h in range(2):
            wait_bytes(ybuf.at[g, h, pl.ds(1, side - 1)], r2_rsem.at[g, h, 0])
            wait_bytes(ybuf.at[g, h, 0, 1 - core], r2_rsem.at[g, h, 1])
            for c in range(CORES):
                total = ybuf[g, h, 0, c]
                for k in range(1, side):
                    total = total + ybuf[g, h, k, c]
                y_ref[:, cols_of(g, h, c)] = total.astype(BF16)

    wait_meta(meta_ssem)
    for h in range(2):
        wait_bytes(xg.at[h, pl.ds(0, side - 1 + 2 * side + side + chips)], ag_ssem.at[h])
    wait_bytes(mbuf.at[:, :, pl.ds(1, side - 1)], r1_ssem.at[0])
    wait_bytes(mbuf.at[:, :, 0, 0], r1_ssem.at[1])
    wait_bytes(pbuf.at[:, :, pl.ds(1, side - 1)], r2_ssem.at[0])
    wait_bytes(pbuf.at[:, :, 0, 0], r2_ssem.at[1])


def solution(mesh):
    num_devices = mesh.shape['ep']
    side = math.isqrt(num_devices // CORES)
    row_spec = P(('dp', 'ep'), None)
    expert_spec = P('ep', None, None)

    def device_step(tokens, routes, w_router, w_one, w_three, w_two):
        num_tokens, d_model = tokens.shape
        top_k = routes.shape[1]
        num_experts = w_router.shape[1]
        local_experts, _, d_expert = w_one.shape
        cap = slot_capacity(num_tokens, top_k, num_experts)
        half = d_model // 2
        piece = half // CORES // 2
        chips = side * side
        any_spec = pl.BlockSpec(memory_space=pl.ANY)
        vmem_spec = pl.BlockSpec(memory_space=pltpu.VMEM)
        dma = pltpu.SemaphoreType.DMA
        return pl.pallas_call(
            functools.partial(moe_kernel, side),
            out_shape=jax.ShapeDtypeStruct((num_tokens, d_model), BF16),
            in_specs=[any_spec, any_spec, any_spec, any_spec, any_spec, any_spec],
            out_specs=vmem_spec,
            scratch_shapes=[
                pltpu.VMEM((2, num_devices, num_tokens, half), BF16),
                pltpu.VMEM((top_k, num_tokens), jnp.int32),
                pltpu.VMEM((d_model, num_experts), BF16),
                pltpu.VMEM((local_experts, 2, d_model, d_expert), BF16),
                pltpu.VMEM((local_experts, d_expert, d_model), BF16),
                pltpu.VMEM((local_experts, side, side, CORES * cap, d_model), BF16),
                pltpu.VMEM((2, chips * CORES * cap, d_expert), BF16),
                pltpu.VMEM((num_devices, top_k, LANES), F32),
                pltpu.VMEM((chips, num_experts, LANES), F32),
                pltpu.VMEM((chips, num_experts, LANES), F32),
                pltpu.VMEM((2, 2, side, CORES, local_experts, side, CORES * cap, piece), BF16),
                pltpu.VMEM((2, 2, side, CORES, num_tokens, piece), F32),
                pltpu.VMEM((2, 2, side, CORES, num_tokens, piece), F32),
                dma, dma, dma, dma((2, local_experts)), dma, dma, dma((2,)), dma((side, side)), dma((side, side)),
                dma((2,)), dma((2, 2, side)), dma((2,)), dma((2, 2, 2)),
            ],
            compiler_params=pltpu.CompilerParams(collective_id=0, has_side_effects=True, vmem_limit_bytes=67043328),
        )(tokens, routes.T, w_router, w_one, w_three, w_two)

    return jax.shard_map(device_step, mesh=mesh, in_specs=(row_spec, row_spec, P(None, None), expert_spec, expert_spec, expert_spec), out_specs=row_spec, check_vma=False)
```

```python
import functools
import math

import jax
import jax.numpy as jnp
from jax import lax
from jax.experimental import pallas as pl
from jax.experimental.pallas import tpu as pltpu
from jax.sharding import PartitionSpec as P

MESH = pl.DeviceIdType.MESH
F32 = jnp.float32
BF16 = jnp.bfloat16
CORES = 2
LANES = 128


def slot_capacity(num_tokens, top_k, num_experts):
    return 8 * ((3 * num_tokens * top_k + 16 * num_experts - 1) // (16 * num_experts))


def moe_kernel(
    side,
    x_hbm, routes_hbm, wr_hbm, w1_hbm, w3_hbm, w2_hbm, y_ref,
    xg, routes_ref, wr, w13, w2, xo, hid, meta, slots, gates, mbuf, pbuf, rbuf, ybuf,
    x_sem, wr_sem, routes_sem, w_sem, meta_ssem, meta_rsem, ag_ssem, ag_rsem, core_rsem,
    r1_ssem, r1_rsem, relay_ssem, relay_rsem, r2_ssem, r2_rsem,
):
    num_devices = CORES * side * side
    chips = side * side
    num_tokens, d_model = x_hbm.shape
    half = d_model // 2
    quarter = half // CORES
    piece = quarter // 2
    local_experts, _, _, d_expert = w13.shape
    chip_experts = CORES * local_experts
    num_experts = num_devices * local_experts
    top_k = routes_ref.shape[0]
    cap = xo.shape[3] // CORES

    me = lax.axis_index('ep')
    core = lax.rem(me, CORES)
    my_x = lax.rem(lax.div(me, CORES), side)
    my_y = lax.div(me, CORES * side)

    def ring(v, k):
        return lax.rem(v + k, side)

    far = side // 2

    def spot(k):
        return k + (k // far) * (side + 1 - 2 * k)

    def chip_at(y, x):
        return y * side + x

    def dev(y, x, c):
        return chip_at(y, x) * CORES + c

    partner = dev(my_y, my_x, 1 - core)

    def remote(src, dst, ssem, rsem, target):
        return pltpu.make_async_remote_copy(src_ref=src, dst_ref=dst, send_sem=ssem, recv_sem=rsem, device_id={'ep': target}, device_id_type=MESH)

    barrier = pltpu.get_barrier_semaphore()

    def greet(i, carry):
        pl.semaphore_signal(barrier, inc=1, device_id={'ep': lax.rem(me + i, num_devices)}, device_id_type=MESH)
        return carry

    lax.fori_loop(1, num_devices, greet, 0)

    x_copies = [pltpu.make_async_copy(x_hbm.at[:, pl.ds(h * half, half)], xg.at[h, me], x_sem) for h in range(2)]
    for cp in x_copies:
        cp.start()
    wr_copy = pltpu.make_async_copy(wr_hbm, wr, wr_sem)
    wr_copy.start()
    routes_copy = pltpu.make_async_copy(routes_hbm, routes_ref, routes_sem)
    routes_copy.start()

    def weight_copies(e):
        return [
            pltpu.make_async_copy(w1_hbm.at[e], w13.at[e, 0], w_sem.at[0, e]),
            pltpu.make_async_copy(w3_hbm.at[e], w13.at[e, 1], w_sem.at[0, e]),
            pltpu.make_async_copy(w2_hbm.at[e], w2.at[e], w_sem.at[1, e]),
        ]

    def start_weights(e, carry):
        for cp in weight_copies(e):
            cp.start()
        return carry

    lax.fori_loop(0, local_experts, start_weights, 0)


    pltpu.make_async_copy(xg.at[:, me], xg.at[:, me], x_sem).wait()

    pl.semaphore_wait(barrier, num_devices - 1)

    def place(h, a, b):
        if h == 0:
            return ring(my_y, b), ring(my_x, a)
        return ring(my_y, a), ring(my_x, b)

    def block_src(h, a, b, c):
        y, x = place(h, a, b)
        return dev(y, x, c)

    def move_block(h, src, rsem, target):
        return remote(xg.at[h, src], xg.at[h, src], ag_ssem.at[h], rsem, target)

    def first_copy(h, k):
        return move_block(h, me, ag_rsem.at[side - k, 0], block_src(h, k, 0, core))

    def first_relay(h):
        k = 1 + core * (side - 2)
        return move_block(h, block_src(h, k, 0, core), ag_rsem.at[side // 2, 0], block_src(h, side - k, 0, core))

    def second_copy(h, a, k):
        return move_block(h, block_src(h, a, 0, core), ag_rsem.at[a, side - k], block_src(h, 0, k, core))

    def relay_copy(h, a, k):
        return move_block(h, block_src(h, a, k, core), ag_rsem.at[a, side // 2], block_src(h, 0, side - k, core))

    def core_copy(h, a, b):
        return move_block(h, block_src(h, a, b, core), core_rsem.at[a, b], partner)

    def wait_blocks(sem):
        pltpu.make_async_copy(xg.at[:, me], xg.at[:, me], sem).wait()

    def meta_copy(i):
        return remote(meta.at[me], meta.at[me], meta_ssem, meta_rsem, lax.rem(me + i, num_devices))

    def send_meta(i, carry):
        meta_copy(i).start()
        return carry

    def wait_meta(sem):
        others = meta.at[pl.ds(0, num_devices - 1)]
        pltpu.make_async_copy(others, others, sem).wait()

    for h in range(2):
        for k in (1, side - 1):
            first_copy(h, k).start()

    wr_copy.wait()
    routes_copy.wait()
    x_local = [xg[h, me] for h in range(2)]
    logits = sum(
        lax.dot_general(wr[pl.ds(h * half, half), :], x_local[h], (((0,), (1,)), ((), ())), preferred_element_type=F32)
        for h in range(2)
    )
    routes = routes_ref[...]
    expert_iota = lax.broadcasted_iota(jnp.int32, (num_experts, num_tokens), 0)
    picked = jnp.concatenate(
        [jnp.sum(jnp.where(expert_iota == routes[j:j + 1, :], logits, 0.0), axis=0, keepdims=True) for j in range(top_k)], axis=0)
    ex = jnp.exp(picked - jnp.max(picked, axis=0, keepdims=True))
    gate = ex / jnp.sum(ex, axis=0, keepdims=True)
    meta[me] = jnp.concatenate([routes.astype(F32) + 1.0, gate], axis=1)

    lax.fori_loop(1, num_devices, send_meta, 0)
    for h in range(2):
        for k in (1, side - 1):
            second_copy(h, 0, k).start()
        core_copy(h, 0, 0).start()

    row_i = lax.broadcasted_iota(jnp.int32, (LANES, LANES), 0)
    col_i = lax.broadcasted_iota(jnp.int32, (LANES, LANES), 1)
    before = jnp.where((row_i < col_i) & (row_i // num_tokens == col_i // num_tokens), 1.0, 0.0).astype(BF16)
    ids = lax.broadcasted_iota(jnp.int32, (num_experts, LANES), 0).astype(F32) + 1.0

    def plan_chip(p, carry):
        tiles = [meta[CORES * p + c] for c in range(CORES)]
        turned = [pltpu.roll(v, num_tokens, 1) for v in tiles]
        low = lax.broadcasted_iota(jnp.int32, tiles[0].shape, 1) < num_tokens
        picks = jnp.where(low, tiles[0], turned[1])
        shares = jnp.where(low, turned[0], tiles[1])
        mask = jnp.zeros((num_experts, LANES), F32)
        weight = jnp.zeros((num_experts, LANES), F32)
        for j in range(top_k):
            hit = ids == picks[j:j + 1, :]
            mask = jnp.where(hit, 1.0, mask)
            weight = jnp.where(hit, shares[j:j + 1, :], weight)
        rank = jnp.dot(mask.astype(BF16), before, preferred_element_type=F32)
        slots[p] = jnp.where(mask > 0.0, rank, -1.0)
        gates[p] = weight
        return carry


    pair_row = lax.broadcasted_iota(jnp.int32, (CORES * cap, LANES), 0)
    pair_lane = lax.broadcasted_iota(jnp.int32, (CORES * cap, LANES), 1)
    wanted = jnp.where(pair_row // cap == pair_lane // num_tokens, pair_row % cap, -2).astype(F32)

    def gather_chip(h, a, b):
        p = chip_at(*place(h, a, b))
        py, px = (spot(b), spot(a)) if h == 0 else (spot(a), spot(b))
        mine = slots[p, pl.ds(me * local_experts, local_experts), :]
        pick = jnp.where(mine[:, None, :] == wanted[None], 1.0, 0.0).reshape(local_experts * CORES * cap, LANES).astype(BF16)
        rows = xg[h, pl.ds(p * CORES, CORES)].reshape(CORES * num_tokens, half)
        out = jnp.dot(pick, rows, preferred_element_type=F32).astype(BF16)
        xo[:, py, px, :, pl.ds(h * half, half)] = out.reshape(local_experts, CORES * cap, half)

    def finish(a, b):
        wait_blocks(core_rsem.at[a, b])
        for h in range(2):
            gather_chip(h, a, b)

    def land(a, b):
        wait_blocks(ag_rsem.at[a, b])
        for h in range(2):
            core_copy(h, a, b).start()

    near = (1, side - 1) + tuple(range(2, side - 1))

    def same_line(a):
        for h in range(2):
            for k in (1, side - 1):
                second_copy(h, a, k).start()

    def relay(a, k):
        for h in range(2):
            relay_copy(h, a, k).start()

    def own_lines(p, carry):
        finish(spot(p), 0)
        return carry

    def near_lines(p, carry):
        finish(spot(p), 1)
        finish(spot(p), side - 1)
        return carry

    def far_lines(p, carry):
        finish(spot(p), far)
        return carry

    for a in near[:2]:
        land(a, 0)
    for h in range(2):
        first_relay(h).start()
    for a in near[:2]:
        same_line(a)
    wait_meta(meta_rsem)
    lax.fori_loop(0, chips, plan_chip, 0)
    land(far, 0)
    same_line(far)
    land(0, 1)
    relay(0, 1)
    land(0, side - 1)
    land(1, 1)
    relay(1, 1)
    land(side - 1, side - 1)
    relay(side - 1, side - 1)
    land(1, side - 1)
    land(side - 1, 1)
    lax.fori_loop(0, side - 1, own_lines, 0)
    lax.fori_loop(0, side - 1, near_lines, 0)
    land(far, side - 1)
    relay(far, side - 1)
    land(far, 1)

    def r1_place(h, k):
        if h == 0:
            return ring(my_y, k), my_x
        return my_y, ring(my_x, k)

    close, edge = pl.ds(0, side - 1), pl.ds(side - 1, 1)
    whole = pl.ds(0, side)
    n_close = (side - 1) * (side - 1) * CORES * cap
    n_rows = chips * CORES * cap
    lines = {
        'near': [(0, close)] + [(k, close) for k in (1, side - 1)],
        'far': [(0, edge)] + [(far, whole)] + [(k, edge) for k in (1, side - 1)],
        'all': [(0, whole)] + [(k, whole) for k in (far, 1, side - 1)],
    }
    spans = {'near': pl.ds(0, n_close), 'far': pl.ds(n_close, n_rows - n_close), 'all': pl.ds(0, n_rows)}

    def read_rows(part, e):
        if part == 'near':
            return xo[e, close, close].reshape(n_close, d_model)
        if part == 'far':
            n_edge = side * CORES * cap
            return jnp.concatenate([xo[e, side - 1].reshape(n_edge, d_model), xo[e, close, side - 1].reshape(n_rows - n_close - n_edge, d_model)], axis=0)
        return xo[e].reshape(n_rows, d_model)

    def write_rows(part, e, cols, o):
        n = o.shape[1]
        if part == 'near':
            xo[e, close, close, :, cols] = o.reshape(side - 1, side - 1, CORES * cap, n)
        elif part == 'far':
            n_edge = side * CORES * cap
            xo[e, side - 1, :, :, cols] = o[:n_edge].reshape(side, CORES * cap, n)
            xo[e, close, side - 1, :, cols] = o[n_edge:].reshape(side - 1, CORES * cap, n)
        else:
            xo[e, :, :, :, cols] = o.reshape(side, side, CORES * cap, n)

    def line_ref(h, e, k, span, cols):
        return xo.at[e, spot(k), span, :, cols] if h == 0 else xo.at[e, span, spot(k), :, cols]

    def cols_of(g, h, c):
        return pl.ds(pl.multiple_of(h * half + c * quarter + g * piece, piece), piece)

    def r1_copy(g, h, e, k, span, cm):
        y, x = r1_place(h, k)
        src = line_ref(h, e, k, span, cols_of(g, h, cm))
        return remote(src, mbuf.at[g, h, k, core, e, span], r1_ssem.at[0], r1_rsem.at[g, h, k], dev(y, x, cm))

    def r1_partner(g, h, e, span):
        src = line_ref(h, e, 0, span, cols_of(g, h, 1 - core))
        return remote(src, mbuf.at[g, h, 0, core, e, span], r1_ssem.at[1], r1_rsem.at[g, h, 0], partner)

    n1 = 256

    def up_rows(part, e):
        if part != 'far':
            pltpu.make_async_copy(w13.at[e], w13.at[e], w_sem.at[0, e]).wait()

        def up(t, carry):
            rows = read_rows(part, e)
            cols = pl.ds(t * n1, n1)
            a = jnp.dot(rows, w13[e, 0, :, cols], preferred_element_type=F32)
            b = jnp.dot(rows, w13[e, 1, :, cols], preferred_element_type=F32)
            hid[e % 2, spans[part], cols] = (a * jax.nn.sigmoid(a) * b).astype(BF16)
            return carry

        for t in range(d_expert // n1):
            up(t, 0)

    def send_rows(part, e, g, h):
        for k, span in lines[part][1:]:
            for cm in range(CORES):
                r1_copy(g, h, e, k, span, cm).start()
        span = lines[part][0][1]
        r1_partner(g, h, e, span).start()
        cols = cols_of(g, h, core)
        mbuf[g, h, 0, core, e, span] = xo[e, 0, span, :, cols] if h == 0 else xo[e, span, 0, :, cols]

    def down_group(part, e, g):
        for h in range(2):
            def down(c, carry):
                cols = cols_of(g, h, c)
                write_rows(part, e, cols, jnp.dot(hid[e % 2, spans[part], :], w2[e, :, cols], preferred_element_type=F32).astype(BF16))
                return carry

            for c in range(CORES):
                down(c, 0)
        for h in range(2):
            send_rows(part, e, g, h)

    def wait_down(e):
        pltpu.make_async_copy(w2.at[e], w2.at[e], w_sem.at[1, e]).wait()

    def down_rows(part, e):
        if part != 'far':
            wait_down(e)

        def down(t, carry):
            cols = pl.ds(t * quarter, quarter)
            write_rows(part, e, cols, jnp.dot(hid[e % 2, spans[part], :], w2[e, :, cols], preferred_element_type=F32).astype(BF16))
            return carry

        for h in range(2):
            for t in range(h * CORES, (h + 1) * CORES):
                down(t, 0)
            for g in range(2):
                send_rows(part, e, g, h)

    early = 2

    def far_expert(e, carry):
        up_rows('far', e)
        down_rows('far', e)
        return carry

    def all_expert(e, carry):
        up_rows('all', e)
        wait_down(e)
        down_group('all', e, 0)
        return carry

    def all_second(e, carry):
        down_group('all', e, 1)
        return carry

    for e in range(early):
        up_rows('near', e)
        if e > 0:
            for p in range((e - 1) * far, e * far):
                land(spot(p), far)
        down_rows('near', e)
    for p in range((early - 1) * far, side):
        land(spot(p), far)
    finish(far, 0)
    finish(far, 1)
    finish(far, side - 1)
    lax.fori_loop(0, side, far_lines, 0)
    lax.fori_loop(0, early, far_expert, 0)
    lax.fori_loop(early, local_experts, all_expert, 0)
    lax.fori_loop(early, local_experts, all_second, 0)

    def r2_place(h, k):
        if h == 0:
            return my_y, ring(my_x, k)
        return ring(my_y, k), my_x

    via = 1 + core * (side - 2)
    direct = side - via

    def sum_place(k):
        return lax.div(k + 1, 2)

    def relay_sums(g, h):
        y, x = r2_place(h, via)
        return remote(pbuf.at[g, h, far], rbuf.at[g, h], relay_ssem, relay_rsem.at[g, h], dev(y, x, core))

    def r2_copy(g, h, k, cd):
        y, x = r2_place(h, k)
        return remote(pbuf.at[g, h, k, cd], ybuf.at[g, h, sum_place(k), core], r2_ssem.at[0], r2_rsem.at[g, h, 0], dev(y, x, cd))

    def r2_partner(g, h):
        return remote(pbuf.at[g, h, 0, 1 - core], ybuf.at[g, h, 0, core], r2_ssem.at[1], r2_rsem.at[g, h, 1], partner)

    def merge(g, h, k):
        y, x = r2_place(h, k)
        p = chip_at(y, x)
        q = spot(k)
        lhs = []
        for j in range(side):
            sy, sx = r1_place(h, side - j)
            base = pl.multiple_of(chip_at(sy, sx) * chip_experts, chip_experts)
            hit = slots[p, pl.ds(base, chip_experts), :][:, None, :] == wanted[None]
            share = gates[p, pl.ds(base, chip_experts), :]
            g_hi = share.astype(BF16).astype(F32)
            g_mid = (share - g_hi).astype(BF16).astype(F32)
            g_lo = share - g_hi - g_mid
            lhs.append(jnp.concatenate([
                jnp.where(hit, v[:, None, :], 0.0).reshape(chip_experts * CORES * cap, LANES).astype(BF16) for v in (g_hi, g_mid, g_lo)], axis=1))
        rows = mbuf[g, h, :, :, :, q].reshape(side * CORES * local_experts * CORES * cap, piece)
        out = lax.dot_general(jnp.concatenate(lhs, axis=0), rows, (((0,), (0,)), ((), ())), preferred_element_type=F32)
        total = out[:LANES] + (out[LANES:2 * LANES] + out[2 * LANES:])
        pbuf[g, h, k] = total.reshape(CORES, num_tokens, piece)

    def wait_bytes(ref, sem):
        pltpu.make_async_copy(ref, ref, sem).wait()

    def pass_on(g):
        for h in range(2):
            wait_bytes(rbuf.at[g, h], relay_rsem.at[g, h])
            pbuf[g, h, via] = pbuf[g, h, via] + rbuf[g, h]
            for cd in range(CORES):
                r2_copy(g, h, via, cd).start()

    def merge_group(g, carry):
        for h in range(2):
            for k in range(1, side):
                wait_bytes(mbuf.at[g, h, k], r1_rsem.at[g, h, k])
            wait_bytes(mbuf.at[g, h, 0, 1 - core], r1_rsem.at[g, h, 0])

        for h in range(2):
            merge(g, h, far)
            relay_sums(g, h).start()

        @pl.when(g > 0)
        def _():
            pass_on(g - 1)

        for h in range(2):
            merge(g, h, direct)
            for cd in range(CORES):
                r2_copy(g, h, direct, cd).start()
        for h in range(2):
            merge(g, h, via)
        for h in range(2):
            merge(g, h, 0)
            r2_partner(g, h).start()
            ybuf[g, h, 0, core] = pbuf[g, h, 0, core]
        return carry

    lax.fori_loop(0, 2, merge_group, 0)
    pass_on(1)

    for g in range(2):
        for h in range(2):
            wait_bytes(ybuf.at[g, h, pl.ds(1, 2)], r2_rsem.at[g, h, 0])
            wait_bytes(ybuf.at[g, h, 0, 1 - core], r2_rsem.at[g, h, 1])
            for c in range(CORES):
                total = ybuf[g, h, 0, c]
                for k in range(1, 3):
                    total = total + ybuf[g, h, k, c]
                y_ref[:, cols_of(g, h, c)] = total.astype(BF16)

    wait_meta(meta_ssem)
    for h in range(2):
        wait_bytes(xg.at[h, pl.ds(0, side - 1 + 2 * side + side + chips)], ag_ssem.at[h])
    wait_bytes(mbuf.at[:, :, pl.ds(1, side - 1)], r1_ssem.at[0])
    wait_bytes(mbuf.at[:, :, 0, 0], r1_ssem.at[1])
    wait_bytes(pbuf.at[:, :, pl.ds(0, 2)], r2_ssem.at[0])
    wait_bytes(rbuf, relay_ssem)
    wait_bytes(pbuf.at[:, :, 0, 0], r2_ssem.at[1])


def solution(mesh):
    num_devices = mesh.shape['ep']
    side = math.isqrt(num_devices // CORES)
    row_spec = P(('dp', 'ep'), None)
    expert_spec = P('ep', None, None)

    def device_step(tokens, routes, w_router, w_one, w_three, w_two):
        num_tokens, d_model = tokens.shape
        top_k = routes.shape[1]
        num_experts = w_router.shape[1]
        local_experts, _, d_expert = w_one.shape
        cap = slot_capacity(num_tokens, top_k, num_experts)
        half = d_model // 2
        piece = half // CORES // 2
        chips = side * side
        any_spec = pl.BlockSpec(memory_space=pl.ANY)
        vmem_spec = pl.BlockSpec(memory_space=pltpu.VMEM)
        dma = pltpu.SemaphoreType.DMA
        return pl.pallas_call(
            functools.partial(moe_kernel, side),
            out_shape=jax.ShapeDtypeStruct((num_tokens, d_model), BF16),
            in_specs=[any_spec, any_spec, any_spec, any_spec, any_spec, any_spec],
            out_specs=vmem_spec,
            scratch_shapes=[
                pltpu.VMEM((2, num_devices, num_tokens, half), BF16),
                pltpu.VMEM((top_k, num_tokens), jnp.int32),
                pltpu.VMEM((d_model, num_experts), BF16),
                pltpu.VMEM((local_experts, 2, d_model, d_expert), BF16),
                pltpu.VMEM((local_experts, d_expert, d_model), BF16),
                pltpu.VMEM((local_experts, side, side, CORES * cap, d_model), BF16),
                pltpu.VMEM((2, chips * CORES * cap, d_expert), BF16),
                pltpu.VMEM((num_devices, top_k, LANES), F32),
                pltpu.VMEM((chips, num_experts, LANES), F32),
                pltpu.VMEM((chips, num_experts, LANES), F32),
                pltpu.VMEM((2, 2, side, CORES, local_experts, side, CORES * cap, piece), BF16),
                pltpu.VMEM((2, 2, side, CORES, num_tokens, piece), F32),
                pltpu.VMEM((2, 2, CORES, num_tokens, piece), F32),
                pltpu.VMEM((2, 2, 3, CORES, num_tokens, piece), F32),
                dma, dma, dma, dma((2, local_experts)), dma, dma, dma((2,)), dma((side, side)), dma((side, side)),
                dma((2,)), dma((2, 2, side)), dma, dma((2, 2)), dma((2,)), dma((2, 2, 2)),
            ],
            compiler_params=pltpu.CompilerParams(collective_id=0, has_side_effects=True, vmem_limit_bytes=67043328),
        )(tokens, routes.T, w_router, w_one, w_three, w_two)

    return jax.shard_map(device_step, mesh=mesh, in_specs=(row_spec, row_spec, P(None, None), expert_spec, expert_spec, expert_spec), out_specs=row_spec, check_vma=False)
```

```python
import functools
import math

import jax
import jax.numpy as jnp
from jax import lax
from jax.experimental import pallas as pl
from jax.experimental.pallas import tpu as pltpu
from jax.sharding import PartitionSpec as P

MESH = pl.DeviceIdType.MESH
F32 = jnp.float32
BF16 = jnp.bfloat16
CORES = 2
LANES = 128


def slot_capacity(num_tokens, top_k, num_experts):
    return 8 * ((3 * num_tokens * top_k + 16 * num_experts - 1) // (16 * num_experts))


def moe_kernel(
    side,
    x_hbm, routes_hbm, wr_hbm, w1_hbm, w3_hbm, w2_hbm, y_ref,
    xg, routes_ref, wr, w13, w2, xo, hid, meta, mine, slots, gates, mbuf, pbuf, rbuf, ybuf,
    x_sem, wr_sem, routes_sem, w_sem, meta_ssem, meta_rsem, ag_ssem, ag_rsem, core_rsem,
    r1_ssem, r1_rsem, relay_ssem, relay_rsem, r2_ssem, r2_rsem,
):
    num_devices = CORES * side * side
    chips = side * side
    num_tokens, d_model = x_hbm.shape
    half = d_model // 2
    quarter = half // CORES
    piece = quarter // 2
    local_experts, _, _, d_expert = w13.shape
    chip_experts = CORES * local_experts
    num_experts = num_devices * local_experts
    top_k = routes_ref.shape[0]
    cap = xo.shape[3] // CORES

    me = lax.axis_index('ep')
    core = lax.rem(me, CORES)
    my_x = lax.rem(lax.div(me, CORES), side)
    my_y = lax.div(me, CORES * side)

    def ring(v, k):
        return lax.rem(v + k, side)

    far = side // 2

    def spot(k):
        return k + (k // far) * (side + 1 - 2 * k)

    def chip_at(y, x):
        return y * side + x

    def dev(y, x, c):
        return chip_at(y, x) * CORES + c

    partner = dev(my_y, my_x, 1 - core)

    def remote(src, dst, ssem, rsem, target):
        return pltpu.make_async_remote_copy(src_ref=src, dst_ref=dst, send_sem=ssem, recv_sem=rsem, device_id={'ep': target}, device_id_type=MESH)

    barrier = pltpu.get_barrier_semaphore()

    peers = [partner]
    for k in range(1, side):
        for c in range(CORES):
            peers += [dev(my_y, ring(my_x, k), c), dev(ring(my_y, k), my_x, c)]
    for peer in peers:
        pl.semaphore_signal(barrier, inc=1, device_id={'ep': peer}, device_id_type=MESH)

    x_copies = [pltpu.make_async_copy(x_hbm.at[:, pl.ds(h * half, half)], xg.at[h, me], x_sem) for h in range(2)]
    for cp in x_copies:
        cp.start()
    wr_copy = pltpu.make_async_copy(wr_hbm, wr, wr_sem)
    wr_copy.start()
    routes_copy = pltpu.make_async_copy(routes_hbm, routes_ref, routes_sem)
    routes_copy.start()

    def weight_copies(e):
        return [
            pltpu.make_async_copy(w1_hbm.at[e], w13.at[e, 0], w_sem.at[0, e]),
            pltpu.make_async_copy(w3_hbm.at[e], w13.at[e, 1], w_sem.at[0, e]),
            pltpu.make_async_copy(w2_hbm.at[e], w2.at[e], w_sem.at[1, e]),
        ]

    def start_weights(e, carry):
        for cp in weight_copies(e):
            cp.start()
        return carry

    lax.fori_loop(0, local_experts, start_weights, 0)


    pltpu.make_async_copy(xg.at[:, me], xg.at[:, me], x_sem).wait()

    pl.semaphore_wait(barrier, len(peers))

    def place(h, a, b):
        if h == 0:
            return ring(my_y, b), ring(my_x, a)
        return ring(my_y, a), ring(my_x, b)

    def block_src(h, a, b, c):
        y, x = place(h, a, b)
        return dev(y, x, c)

    def move_block(h, src, rsem, target):
        return remote(xg.at[h, src], xg.at[h, src], ag_ssem.at[h], rsem, target)

    def first_copy(h, k):
        return move_block(h, me, ag_rsem.at[side - k, 0], block_src(h, k, 0, core))

    def first_relay(h):
        k = 1 + core * (side - 2)
        return move_block(h, block_src(h, k, 0, core), ag_rsem.at[side // 2, 0], block_src(h, side - k, 0, core))

    def second_copy(h, a, k):
        return move_block(h, block_src(h, a, 0, core), ag_rsem.at[a, side - k], block_src(h, 0, k, core))

    def relay_copy(h, a, k):
        return move_block(h, block_src(h, a, k, core), ag_rsem.at[a, side // 2], block_src(h, 0, side - k, core))

    def core_copy(h, a, b):
        return move_block(h, block_src(h, a, b, core), core_rsem.at[a, b], partner)

    def wait_blocks(sem):
        pltpu.make_async_copy(xg.at[:, me], xg.at[:, me], sem).wait()

    def meta_copy(stage, k):
        ref = (meta.at[my_y, my_x, core], meta.at[my_y, :, core], meta.at[:, :, core])[stage]
        target = (dev(my_y, ring(my_x, k), core), dev(ring(my_y, k), my_x, core), partner)[stage]
        return remote(ref, ref, meta_ssem.at[stage], meta_rsem.at[stage], target)

    def wait_meta(stage, sem):
        ref = (meta.at[0, pl.ds(0, side - 1), 0], meta.at[pl.ds(0, side - 1), :, 0], meta.at[:, :, 0])[stage]
        pltpu.make_async_copy(ref, ref, sem.at[stage]).wait()

    for h in range(2):
        for k in (1, side - 1):
            first_copy(h, k).start()

    wr_copy.wait()
    routes_copy.wait()
    x_local = [xg[h, me] for h in range(2)]
    logits = sum(
        lax.dot_general(wr[pl.ds(h * half, half), :], x_local[h], (((0,), (1,)), ((), ())), preferred_element_type=F32)
        for h in range(2)
    )
    routes = routes_ref[...]
    expert_iota = lax.broadcasted_iota(jnp.int32, (num_experts, num_tokens), 0)
    picked = jnp.concatenate(
        [jnp.sum(jnp.where(expert_iota == routes[j:j + 1, :], logits, 0.0), axis=0, keepdims=True) for j in range(top_k)], axis=0)
    ex = jnp.exp(picked - jnp.max(picked, axis=0, keepdims=True))
    gate = ex / jnp.sum(ex, axis=0, keepdims=True)
    meta[my_y, my_x, core] = jnp.concatenate([routes.astype(F32) + 1.0, gate], axis=1)

    for k in range(1, side):
        meta_copy(0, k).start()
    for h in range(2):
        for k in (1, side - 1):
            second_copy(h, 0, k).start()
        core_copy(h, 0, 0).start()

    row_i = lax.broadcasted_iota(jnp.int32, (LANES, LANES), 0)
    col_i = lax.broadcasted_iota(jnp.int32, (LANES, LANES), 1)
    before = jnp.where((row_i < col_i) & (row_i // num_tokens == col_i // num_tokens), 1.0, 0.0).astype(BF16)
    tile_ids = lax.broadcasted_iota(jnp.int32, (chip_experts, LANES), 0) + 1

    def chip_ids(y, x):
        return (tile_ids + chip_at(y, x) * chip_experts).astype(F32)

    def chip_routes(y, x):
        tiles = [meta[y, x, c] for c in range(CORES)]
        turned = [pltpu.roll(v, num_tokens, 1) for v in tiles]
        low = lax.broadcasted_iota(jnp.int32, tiles[0].shape, 1) < num_tokens
        return jnp.where(low, tiles[0], turned[1]), jnp.where(low, turned[0], tiles[1])

    def slots_of(mask):
        rank = jnp.dot(mask.astype(BF16), before, preferred_element_type=F32)
        return jnp.where(mask > 0.0, rank, -1.0)

    my_ids = chip_ids(my_y, my_x)

    def plan_gather(y, carry):
        for x in range(side):
            picks, _ = chip_routes(y, x)
            mask = jnp.zeros((chip_experts, LANES), F32)
            for j in range(top_k):
                mask = jnp.where(my_ids == picks[j:j + 1, :], 1.0, mask)
            mine[y, x] = mask
        return carry

    def plan_merge(k, carry):
        for h in range(2):
            ids = jnp.concatenate([chip_ids(*r1_place(h, side - j)) for j in range(side)], axis=0)
            picks, shares = chip_routes(*r2_place(h, k))
            mask = jnp.zeros(ids.shape, F32)
            weight = jnp.zeros(ids.shape, F32)
            for j in range(top_k):
                hit = ids == picks[j:j + 1, :]
                mask = jnp.where(hit, 1.0, mask)
                weight = jnp.where(hit, shares[j:j + 1, :], weight)
            slots[h, k] = slots_of(mask)
            gates[h, k] = weight
        return carry

    def r1_place(h, k):
        if h == 0:
            return ring(my_y, k), my_x
        return my_y, ring(my_x, k)

    def r2_place(h, k):
        if h == 0:
            return my_y, ring(my_x, k)
        return ring(my_y, k), my_x

    pair_row = lax.broadcasted_iota(jnp.int32, (CORES * cap, LANES), 0)
    pair_lane = lax.broadcasted_iota(jnp.int32, (CORES * cap, LANES), 1)
    wanted = jnp.where(pair_row // cap == pair_lane // num_tokens, pair_row % cap, -2).astype(F32)

    def gather_chip(h, a, b):
        p = chip_at(*place(h, a, b))
        py, px = (spot(b), spot(a)) if h == 0 else (spot(a), spot(b))
        found = mine[place(h, a, b)[0], place(h, a, b)[1], pl.ds(core * local_experts, local_experts), :]
        pick = jnp.where(found[:, None, :] == wanted[None], 1.0, 0.0).reshape(local_experts * CORES * cap, LANES).astype(BF16)
        rows = xg[h, pl.ds(p * CORES, CORES)].reshape(CORES * num_tokens, half)
        out = jnp.dot(pick, rows, preferred_element_type=F32).astype(BF16)
        xo[:, py, px, :, pl.ds(h * half, half)] = out.reshape(local_experts, CORES * cap, half)

    def finish(a, b):
        wait_blocks(core_rsem.at[a, b])
        for h in range(2):
            gather_chip(h, a, b)

    def land(a, b):
        wait_blocks(ag_rsem.at[a, b])
        for h in range(2):
            core_copy(h, a, b).start()

    near = (1, side - 1) + tuple(range(2, side - 1))

    def same_line(a):
        for h in range(2):
            for k in (1, side - 1):
                second_copy(h, a, k).start()

    def relay(a, k):
        for h in range(2):
            relay_copy(h, a, k).start()

    def own_lines(p, carry):
        finish(spot(p), 0)
        return carry

    def near_lines(p, carry):
        finish(spot(p), 1)
        finish(spot(p), side - 1)
        return carry

    def far_lines(p, carry):
        finish(spot(p), far)
        return carry

    for a in near[:2]:
        land(a, 0)
    for h in range(2):
        first_relay(h).start()
    wait_meta(0, meta_rsem)
    for k in range(1, side):
        meta_copy(1, k).start()
    for a in near[:2]:
        same_line(a)
    land(0, 1)
    relay(0, 1)
    land(0, side - 1)
    wait_meta(1, meta_rsem)
    meta_copy(2, 0).start()
    land(far, 0)
    same_line(far)
    wait_meta(2, meta_rsem)
    lax.fori_loop(0, side, plan_gather, 0)
    mine[...] = slots_of(mine[...].reshape(chips * chip_experts, LANES)).reshape(side, side, chip_experts, LANES)
    lax.fori_loop(0, side, plan_merge, 0)
    land(1, 1)
    relay(1, 1)
    land(side - 1, side - 1)
    relay(side - 1, side - 1)
    land(1, side - 1)
    land(side - 1, 1)
    lax.fori_loop(0, side - 1, own_lines, 0)
    lax.fori_loop(0, side - 1, near_lines, 0)
    land(far, side - 1)
    relay(far, side - 1)

    close, edge = pl.ds(0, side - 1), pl.ds(side - 1, 1)
    whole = pl.ds(0, side)
    n_close = (side - 1) * (side - 1) * CORES * cap
    n_rows = chips * CORES * cap
    lines = {
        'near': [(0, close)] + [(k, close) for k in (1, side - 1)],
        'far': [(0, edge)] + [(far, whole)] + [(k, edge) for k in (1, side - 1)],
        'all': [(0, whole)] + [(k, whole) for k in (far, 1, side - 1)],
    }
    spans = {'near': pl.ds(0, n_close), 'far': pl.ds(n_close, n_rows - n_close), 'all': pl.ds(0, n_rows)}

    def read_rows(part, e):
        if part == 'near':
            return xo[e, close, close].reshape(n_close, d_model)
        if part == 'far':
            n_edge = side * CORES * cap
            return jnp.concatenate([xo[e, side - 1].reshape(n_edge, d_model), xo[e, close, side - 1].reshape(n_rows - n_close - n_edge, d_model)], axis=0)
        return xo[e].reshape(n_rows, d_model)

    def write_rows(part, e, cols, o):
        n = o.shape[1]
        if part == 'near':
            xo[e, close, close, :, cols] = o.reshape(side - 1, side - 1, CORES * cap, n)
        elif part == 'far':
            n_edge = side * CORES * cap
            xo[e, side - 1, :, :, cols] = o[:n_edge].reshape(side, CORES * cap, n)
            xo[e, close, side - 1, :, cols] = o[n_edge:].reshape(side - 1, CORES * cap, n)
        else:
            xo[e, :, :, :, cols] = o.reshape(side, side, CORES * cap, n)

    def line_ref(h, e, k, span, cols):
        return xo.at[e, spot(k), span, :, cols] if h == 0 else xo.at[e, span, spot(k), :, cols]

    def cols_of(g, h, c):
        return pl.ds(pl.multiple_of(h * half + c * quarter + g * piece, piece), piece)

    def r1_copy(g, h, e, k, span, cm):
        y, x = r1_place(h, k)
        src = line_ref(h, e, k, span, cols_of(g, h, cm))
        return remote(src, mbuf.at[g, h, k, core, e, span], r1_ssem.at[0], r1_rsem.at[g, 0], dev(y, x, cm))

    def r1_partner(g, h, e, span):
        src = line_ref(h, e, 0, span, cols_of(g, h, 1 - core))
        return remote(src, mbuf.at[g, h, 0, core, e, span], r1_ssem.at[1], r1_rsem.at[g, 1], partner)

    n1 = 256

    def up_rows(part, e):
        if part != 'far':
            pltpu.make_async_copy(w13.at[e], w13.at[e], w_sem.at[0, e]).wait()

        def up(t, carry):
            rows = read_rows(part, e)
            cols = pl.ds(t * n1, n1)
            a = jnp.dot(rows, w13[e, 0, :, cols], preferred_element_type=F32)
            b = jnp.dot(rows, w13[e, 1, :, cols], preferred_element_type=F32)
            hid[e % 2, spans[part], cols] = (a * jax.nn.sigmoid(a) * b).astype(BF16)
            return carry

        for t in range(d_expert // n1):
            up(t, 0)

    def send_rows(part, e, g, h):
        for k, span in lines[part][1:]:
            for cm in range(CORES):
                r1_copy(g, h, e, k, span, cm).start()
        span = lines[part][0][1]
        r1_partner(g, h, e, span).start()
        cols = cols_of(g, h, core)
        mbuf[g, h, 0, core, e, span] = xo[e, 0, span, :, cols] if h == 0 else xo[e, span, 0, :, cols]

    def down_group(part, e, g):
        for h in range(2):
            def down(c, carry):
                cols = cols_of(g, h, c)
                write_rows(part, e, cols, jnp.dot(hid[e % 2, spans[part], :], w2[e, :, cols], preferred_element_type=F32).astype(BF16))
                return carry

            for c in range(CORES):
                down(c, 0)
        for h in range(2):
            send_rows(part, e, g, h)

    def wait_down(e):
        pltpu.make_async_copy(w2.at[e], w2.at[e], w_sem.at[1, e]).wait()

    def down_rows(part, e):
        if part != 'far':
            wait_down(e)

        def down(t, carry):
            cols = pl.ds(t * quarter, quarter)
            write_rows(part, e, cols, jnp.dot(hid[e % 2, spans[part], :], w2[e, :, cols], preferred_element_type=F32).astype(BF16))
            return carry

        for h in range(2):
            for t in range(h * CORES, (h + 1) * CORES):
                down(t, 0)
            for g in range(2):
                send_rows(part, e, g, h)

    early = 2

    def far_expert(e, carry):
        up_rows('far', e)
        down_rows('far', e)
        return carry

    def all_expert(e, carry):
        up_rows('all', e)
        wait_down(e)
        down_group('all', e, 0)
        return carry

    def all_second(e, carry):
        down_group('all', e, 1)
        return carry

    up_rows('near', 0)
    land(far, 1)
    down_rows('near', 0)
    land(0, far)
    up_rows('near', 1)
    land(1, far)
    land(side - 1, far)
    down_rows('near', 1)
    land(far, far)
    finish(far, 0)
    finish(far, 1)
    finish(far, side - 1)
    lax.fori_loop(0, side, far_lines, 0)
    lax.fori_loop(0, early, far_expert, 0)
    lax.fori_loop(early, local_experts, all_expert, 0)
    lax.fori_loop(early, local_experts, all_second, 0)

    via = 1 + core * (side - 2)
    direct = side - via

    def sum_place(k):
        return lax.div(k + 1, 2)

    def relay_sums(g, h):
        y, x = r2_place(h, via)
        return remote(pbuf.at[g, h, far], rbuf.at[g, h], relay_ssem, relay_rsem.at[g, h], dev(y, x, core))

    def r2_copy(g, h, k, cd):
        y, x = r2_place(h, k)
        return remote(pbuf.at[g, h, k, cd], ybuf.at[g, h, sum_place(k), core], r2_ssem.at[0], r2_rsem.at[g, 0], dev(y, x, cd))

    def r2_partner(g, h):
        return remote(pbuf.at[g, h, 0, 1 - core], ybuf.at[g, h, 0, core], r2_ssem.at[1], r2_rsem.at[g, 1], partner)

    def merge(g, h, k):
        q = spot(k)
        lhs = []
        for j in range(side):
            span = pl.ds(j * chip_experts, chip_experts)
            hit = slots[h, k, span, :][:, None, :] == wanted[None]
            share = gates[h, k, span, :]
            g_hi = share.astype(BF16).astype(F32)
            g_mid = (share - g_hi).astype(BF16).astype(F32)
            g_lo = share - g_hi - g_mid
            lhs.append(jnp.concatenate([
                jnp.where(hit, v[:, None, :], 0.0).reshape(chip_experts * CORES * cap, LANES).astype(BF16) for v in (g_hi, g_mid, g_lo)], axis=1))
        rows = mbuf[g, h, :, :, :, q].reshape(side * CORES * local_experts * CORES * cap, piece)
        out = lax.dot_general(jnp.concatenate(lhs, axis=0), rows, (((0,), (0,)), ((), ())), preferred_element_type=F32)
        total = out[:LANES] + (out[LANES:2 * LANES] + out[2 * LANES:])
        pbuf[g, h, k] = total.reshape(CORES, num_tokens, piece)

    def wait_bytes(ref, sem):
        pltpu.make_async_copy(ref, ref, sem).wait()

    def pass_on(g):
        for h in range(2):
            wait_bytes(rbuf.at[g, h], relay_rsem.at[g, h])
            pbuf[g, h, via] = pbuf[g, h, via] + rbuf[g, h]
            for cd in range(CORES):
                r2_copy(g, h, via, cd).start()

    def merge_group(g, carry):
        wait_bytes(mbuf.at[g, :, pl.ds(1, side - 1)], r1_rsem.at[g, 0])
        wait_bytes(mbuf.at[g, :, 0, 1 - core], r1_rsem.at[g, 1])

        for h in range(2):
            merge(g, h, far)
            relay_sums(g, h).start()

        @pl.when(g > 0)
        def _():
            pass_on(g - 1)

        for h in range(2):
            merge(g, h, direct)
            for cd in range(CORES):
                r2_copy(g, h, direct, cd).start()
        for h in range(2):
            merge(g, h, via)
        for h in range(2):
            merge(g, h, 0)
            r2_partner(g, h).start()
            ybuf[g, h, 0, core] = pbuf[g, h, 0, core]
        return carry

    lax.fori_loop(0, 2, merge_group, 0)
    pass_on(1)

    for g in range(2):
        wait_bytes(ybuf.at[g, :, pl.ds(1, 2)], r2_rsem.at[g, 0])
        wait_bytes(ybuf.at[g, :, 0, 1 - core], r2_rsem.at[g, 1])
        for h in range(2):
            for c in range(CORES):
                total = ybuf[g, h, 0, c]
                for k in range(1, 3):
                    total = total + ybuf[g, h, k, c]
                y_ref[:, cols_of(g, h, c)] = total.astype(BF16)

    for stage in range(3):
        wait_meta(stage, meta_ssem)
    for h in range(2):
        wait_bytes(xg.at[h, pl.ds(0, side - 1 + 2 * side + side + chips)], ag_ssem.at[h])
    wait_bytes(mbuf.at[:, :, pl.ds(1, side - 1)], r1_ssem.at[0])
    wait_bytes(mbuf.at[:, :, 0, 0], r1_ssem.at[1])
    wait_bytes(pbuf.at[:, :, pl.ds(0, 2)], r2_ssem.at[0])
    wait_bytes(rbuf, relay_ssem)
    wait_bytes(pbuf.at[:, :, 0, 0], r2_ssem.at[1])


def solution(mesh):
    num_devices = mesh.shape['ep']
    side = math.isqrt(num_devices // CORES)
    row_spec = P(('dp', 'ep'), None)
    expert_spec = P('ep', None, None)

    def device_step(tokens, routes, w_router, w_one, w_three, w_two):
        num_tokens, d_model = tokens.shape
        top_k = routes.shape[1]
        num_experts = w_router.shape[1]
        local_experts, _, d_expert = w_one.shape
        cap = slot_capacity(num_tokens, top_k, num_experts)
        half = d_model // 2
        piece = half // CORES // 2
        chips = side * side
        any_spec = pl.BlockSpec(memory_space=pl.ANY)
        vmem_spec = pl.BlockSpec(memory_space=pltpu.VMEM)
        dma = pltpu.SemaphoreType.DMA
        return pl.pallas_call(
            functools.partial(moe_kernel, side),
            out_shape=jax.ShapeDtypeStruct((num_tokens, d_model), BF16),
            in_specs=[any_spec, any_spec, any_spec, any_spec, any_spec, any_spec],
            out_specs=vmem_spec,
            scratch_shapes=[
                pltpu.VMEM((2, num_devices, num_tokens, half), BF16),
                pltpu.VMEM((top_k, num_tokens), jnp.int32),
                pltpu.VMEM((d_model, num_experts), BF16),
                pltpu.VMEM((local_experts, 2, d_model, d_expert), BF16),
                pltpu.VMEM((local_experts, d_expert, d_model), BF16),
                pltpu.VMEM((local_experts, side, side, CORES * cap, d_model), BF16),
                pltpu.VMEM((2, chips * CORES * cap, d_expert), BF16),
                pltpu.VMEM((side, side, CORES, top_k, LANES), F32),
                pltpu.VMEM((side, side, CORES * local_experts, LANES), F32),
                pltpu.VMEM((2, side, side * CORES * local_experts, LANES), F32),
                pltpu.VMEM((2, side, side * CORES * local_experts, LANES), F32),
                pltpu.VMEM((2, 2, side, CORES, local_experts, side, CORES * cap, piece), BF16),
                pltpu.VMEM((2, 2, side, CORES, num_tokens, piece), F32),
                pltpu.VMEM((2, 2, CORES, num_tokens, piece), F32),
                pltpu.VMEM((2, 2, 3, CORES, num_tokens, piece), F32),
                dma, dma, dma, dma((2, local_experts)), dma((3,)), dma((3,)), dma((2,)), dma((side, side)), dma((side, side)),
                dma((2,)), dma((2, 2)), dma, dma((2, 2)), dma((2,)), dma((2, 2)),
            ],
            compiler_params=pltpu.CompilerParams(collective_id=0, has_side_effects=True, vmem_limit_bytes=67043328),
        )(tokens, routes.T, w_router, w_one, w_three, w_two)

    return jax.shard_map(device_step, mesh=mesh, in_specs=(row_spec, row_spec, P(None, None), expert_spec, expert_spec, expert_spec), out_specs=row_spec, check_vma=False)
```

```python
import functools
import math

import jax
import jax.numpy as jnp
from jax import lax
from jax.experimental import pallas as pl
from jax.experimental.pallas import tpu as pltpu
from jax.sharding import PartitionSpec as P

MESH = pl.DeviceIdType.MESH
F32 = jnp.float32
BF16 = jnp.bfloat16
CORES = 2
LANES = 128


def slot_capacity(num_tokens, top_k, num_experts):
    return 8 * ((3 * num_tokens * top_k + 16 * num_experts - 1) // (16 * num_experts))


def moe_kernel(
    side,
    x_hbm, routes_hbm, wr_hbm, w1_hbm, w3_hbm, w2_hbm, y_ref,
    xg, routes_ref, wr, w13, w2, xo, hid, meta, mine, slots, gates, mbuf, pbuf, rbuf, ybuf,
    x_sem, wr_sem, routes_sem, w_sem, meta_ssem, meta_rsem, ag_ssem, ag_rsem, core_rsem,
    r1_ssem, r1_rsem, relay_ssem, relay_rsem, r2_ssem, r2_rsem,
):
    num_devices = CORES * side * side
    chips = side * side
    num_tokens, d_model = x_hbm.shape
    half = d_model // 2
    quarter = half // CORES
    piece = quarter // 2
    local_experts, _, _, d_expert = w13.shape
    chip_experts = CORES * local_experts
    num_experts = num_devices * local_experts
    top_k = routes_ref.shape[0]
    cap = xo.shape[3] // CORES

    me = lax.axis_index('ep')
    core = lax.rem(me, CORES)
    my_x = lax.rem(lax.div(me, CORES), side)
    my_y = lax.div(me, CORES * side)

    def ring(v, k):
        return lax.rem(v + k, side)

    far = side // 2

    def spot(k):
        return k + (k // far) * (side + 1 - 2 * k)

    def chip_at(y, x):
        return y * side + x

    def dev(y, x, c):
        return chip_at(y, x) * CORES + c

    partner = dev(my_y, my_x, 1 - core)

    def remote(src, dst, ssem, rsem, target):
        return pltpu.make_async_remote_copy(src_ref=src, dst_ref=dst, send_sem=ssem, recv_sem=rsem, device_id={'ep': target}, device_id_type=MESH)

    barrier = pltpu.get_barrier_semaphore()

    peers = [partner]
    for k in range(1, side):
        for c in range(CORES):
            peers += [dev(my_y, ring(my_x, k), c), dev(ring(my_y, k), my_x, c)]
    for peer in peers:
        pl.semaphore_signal(barrier, inc=1, device_id={'ep': peer}, device_id_type=MESH)

    x_copies = [pltpu.make_async_copy(x_hbm.at[:, pl.ds(h * half, half)], xg.at[h, me], x_sem) for h in range(2)]
    for cp in x_copies:
        cp.start()
    wr_copy = pltpu.make_async_copy(wr_hbm, wr, wr_sem)
    wr_copy.start()
    routes_copy = pltpu.make_async_copy(routes_hbm, routes_ref, routes_sem)
    routes_copy.start()

    def weight_copies(e):
        return [
            pltpu.make_async_copy(w1_hbm.at[e], w13.at[e, 0], w_sem.at[0, e]),
            pltpu.make_async_copy(w3_hbm.at[e], w13.at[e, 1], w_sem.at[0, e]),
            pltpu.make_async_copy(w2_hbm.at[e], w2.at[e], w_sem.at[1, e]),
        ]

    def start_weights(e, carry):
        for cp in weight_copies(e):
            cp.start()
        return carry

    lax.fori_loop(0, local_experts, start_weights, 0)


    pltpu.make_async_copy(xg.at[:, me], xg.at[:, me], x_sem).wait()

    pl.semaphore_wait(barrier, len(peers))

    def place(h, a, b):
        if h == 0:
            return ring(my_y, b), ring(my_x, a)
        return ring(my_y, a), ring(my_x, b)

    def block_src(h, a, b, c):
        y, x = place(h, a, b)
        return dev(y, x, c)

    def move_block(h, src, rsem, target):
        return remote(xg.at[h, src], xg.at[h, src], ag_ssem.at[h], rsem, target)

    def first_copy(h, k):
        return move_block(h, me, ag_rsem.at[side - k, 0], block_src(h, k, 0, core))

    def first_relay(h):
        k = 1 + core * (side - 2)
        return move_block(h, block_src(h, k, 0, core), ag_rsem.at[side // 2, 0], block_src(h, side - k, 0, core))

    def second_copy(h, a, k):
        return move_block(h, block_src(h, a, 0, core), ag_rsem.at[a, side - k], block_src(h, 0, k, core))

    def relay_copy(h, a, k):
        return move_block(h, block_src(h, a, k, core), ag_rsem.at[a, side // 2], block_src(h, 0, side - k, core))

    def core_copy(h, a, b):
        return move_block(h, block_src(h, a, b, core), core_rsem.at[a, 1 if b == side - 1 else b], partner)

    def wait_blocks(sem):
        pltpu.make_async_copy(xg.at[:, me], xg.at[:, me], sem).wait()

    def meta_copy(stage, k):
        ref = (meta.at[my_y, my_x, core], meta.at[my_y, :, core], meta.at[:, :, core])[stage]
        target = (dev(my_y, ring(my_x, k), core), dev(ring(my_y, k), my_x, core), partner)[stage]
        return remote(ref, ref, meta_ssem.at[stage], meta_rsem.at[stage], target)

    def wait_meta(stage, sem):
        ref = (meta.at[0, pl.ds(0, side - 1), 0], meta.at[pl.ds(0, side - 1), :, 0], meta.at[:, :, 0])[stage]
        pltpu.make_async_copy(ref, ref, sem.at[stage]).wait()

    for h in range(2):
        for k in (1, side - 1):
            first_copy(h, k).start()

    wr_copy.wait()
    routes_copy.wait()
    x_local = [xg[h, me] for h in range(2)]
    logits = sum(
        lax.dot_general(wr[pl.ds(h * half, half), :], x_local[h], (((0,), (1,)), ((), ())), preferred_element_type=F32)
        for h in range(2)
    )
    routes = routes_ref[...]
    expert_iota = lax.broadcasted_iota(jnp.int32, (num_experts, num_tokens), 0)
    picked = jnp.concatenate(
        [jnp.sum(jnp.where(expert_iota == routes[j:j + 1, :], logits, 0.0), axis=0, keepdims=True) for j in range(top_k)], axis=0)
    ex = jnp.exp(picked - jnp.max(picked, axis=0, keepdims=True))
    gate = ex / jnp.sum(ex, axis=0, keepdims=True)
    meta[my_y, my_x, core] = jnp.concatenate([routes.astype(F32) + 1.0, gate], axis=1)

    for k in range(1, side):
        meta_copy(0, k).start()
    for h in range(2):
        for k in (1, side - 1):
            second_copy(h, 0, k).start()
        core_copy(h, 0, 0).start()

    row_i = lax.broadcasted_iota(jnp.int32, (LANES, LANES), 0)
    col_i = lax.broadcasted_iota(jnp.int32, (LANES, LANES), 1)
    before = jnp.where((row_i < col_i) & (row_i // num_tokens == col_i // num_tokens), 1.0, 0.0).astype(BF16)
    tile_ids = lax.broadcasted_iota(jnp.int32, (chip_experts, LANES), 0) + 1

    def chip_ids(y, x):
        return (tile_ids + chip_at(y, x) * chip_experts).astype(F32)

    def chip_routes(y, x):
        tiles = [meta[y, x, c] for c in range(CORES)]
        turned = [pltpu.roll(v, num_tokens, 1) for v in tiles]
        low = lax.broadcasted_iota(jnp.int32, tiles[0].shape, 1) < num_tokens
        return jnp.where(low, tiles[0], turned[1]), jnp.where(low, turned[0], tiles[1])

    def slots_of(mask):
        rank = jnp.dot(mask.astype(BF16), before, preferred_element_type=F32)
        return jnp.where(mask > 0.0, rank, -1.0)

    my_ids = chip_ids(my_y, my_x)

    def plan_gather(y, carry):
        for x in range(side):
            picks, _ = chip_routes(y, x)
            mask = jnp.zeros((chip_experts, LANES), F32)
            for j in range(top_k):
                mask = jnp.where(my_ids == picks[j:j + 1, :], 1.0, mask)
            mine[y, x] = mask
        return carry

    def plan_merge(k, carry):
        for h in range(2):
            ids = jnp.concatenate([chip_ids(*r1_place(h, side - j)) for j in range(side)], axis=0)
            picks, shares = chip_routes(*r2_place(h, k))
            mask = jnp.zeros(ids.shape, F32)
            weight = jnp.zeros(ids.shape, F32)
            for j in range(top_k):
                hit = ids == picks[j:j + 1, :]
                mask = jnp.where(hit, 1.0, mask)
                weight = jnp.where(hit, shares[j:j + 1, :], weight)
            slots[h, k] = slots_of(mask)
            gates[h, k] = weight
        return carry

    def r1_place(h, k):
        if h == 0:
            return ring(my_y, k), my_x
        return my_y, ring(my_x, k)

    def r2_place(h, k):
        if h == 0:
            return my_y, ring(my_x, k)
        return ring(my_y, k), my_x

    pair_row = lax.broadcasted_iota(jnp.int32, (CORES * cap, LANES), 0)
    pair_lane = lax.broadcasted_iota(jnp.int32, (CORES * cap, LANES), 1)
    wanted = jnp.where(pair_row // cap == pair_lane // num_tokens, pair_row % cap, -2).astype(F32)

    def gather_chip(h, a, b):
        p = chip_at(*place(h, a, b))
        py, px = (spot(b), spot(a)) if h == 0 else (spot(a), spot(b))
        found = mine[place(h, a, b)[0], place(h, a, b)[1], pl.ds(core * local_experts, local_experts), :]
        pick = jnp.where(found[:, None, :] == wanted[None], 1.0, 0.0).reshape(local_experts * CORES * cap, LANES).astype(BF16)
        rows = xg[h, pl.ds(p * CORES, CORES)].reshape(CORES * num_tokens, half)
        out = jnp.dot(pick, rows, preferred_element_type=F32).astype(BF16)
        xo[:, py, px, :, pl.ds(h * half, half)] = out.reshape(local_experts, CORES * cap, half)

    def pick_rows(a, b):
        for h in range(2):
            gather_chip(h, a, b)

    def finish(a, b):
        wait_blocks(core_rsem.at[a, b])
        pick_rows(a, b)

    def finish_near(a):
        four = xg.at[:, pl.ds(0, 2)]
        pltpu.make_async_copy(four, four, core_rsem.at[a, 1]).wait()
        pick_rows(a, 1)
        pick_rows(a, side - 1)

    def arrive(a, b):
        wait_blocks(ag_rsem.at[a, b])

    def share(a, b):
        for h in range(2):
            core_copy(h, a, b).start()

    def land(a, b):
        arrive(a, b)
        share(a, b)

    near = (1, side - 1) + tuple(range(2, side - 1))

    def same_line(a):
        for h in range(2):
            for k in (1, side - 1):
                second_copy(h, a, k).start()

    def relay(a, k):
        for h in range(2):
            relay_copy(h, a, k).start()

    def own_lines(p, carry):
        finish(spot(p), 0)
        return carry

    def near_lines(p, carry):
        finish_near(spot(p))
        return carry

    def far_lines(p, carry):
        finish(spot(p), far)
        return carry

    for a in near[:2]:
        arrive(a, 0)
    for h in range(2):
        first_relay(h).start()
    wait_meta(0, meta_rsem)
    for k in range(1, side):
        meta_copy(1, k).start()
    for a in near[:2]:
        same_line(a)
    for a in near[:2]:
        share(a, 0)
    arrive(0, 1)
    relay(0, 1)
    share(0, 1)
    land(0, side - 1)
    arrive(far, 0)
    same_line(far)
    share(far, 0)
    wait_meta(1, meta_rsem)
    meta_copy(2, 0).start()
    wait_meta(2, meta_rsem)
    lax.fori_loop(0, side, plan_gather, 0)
    mine[...] = slots_of(mine[...].reshape(chips * chip_experts, LANES)).reshape(side, side, chip_experts, LANES)
    lax.fori_loop(0, side, plan_merge, 0)
    arrive(1, 1)
    relay(1, 1)
    share(1, 1)
    arrive(side - 1, side - 1)
    relay(side - 1, side - 1)
    share(side - 1, side - 1)
    land(1, side - 1)
    land(side - 1, 1)
    lax.fori_loop(0, side - 1, own_lines, 0)
    lax.fori_loop(0, side - 1, near_lines, 0)
    arrive(far, side - 1)
    relay(far, side - 1)
    share(far, side - 1)

    close, edge = pl.ds(0, side - 1), pl.ds(side - 1, 1)
    whole = pl.ds(0, side)
    n_close = (side - 1) * (side - 1) * CORES * cap
    n_rows = chips * CORES * cap
    lines = {
        'near': [(0, close)] + [(k, close) for k in (1, side - 1)],
        'far': [(0, edge)] + [(far, whole)] + [(k, edge) for k in (1, side - 1)],
        'all': [(0, whole)] + [(k, whole) for k in (far, 1, side - 1)],
    }
    spans = {'near': pl.ds(0, n_close), 'far': pl.ds(n_close, n_rows - n_close), 'all': pl.ds(0, n_rows)}

    def read_rows(part, e):
        if part == 'near':
            return xo[e, close, close].reshape(n_close, d_model)
        if part == 'far':
            n_edge = side * CORES * cap
            return jnp.concatenate([xo[e, side - 1].reshape(n_edge, d_model), xo[e, close, side - 1].reshape(n_rows - n_close - n_edge, d_model)], axis=0)
        return xo[e].reshape(n_rows, d_model)

    def write_rows(part, e, cols, o):
        n = o.shape[1]
        if part == 'near':
            xo[e, close, close, :, cols] = o.reshape(side - 1, side - 1, CORES * cap, n)
        elif part == 'far':
            n_edge = side * CORES * cap
            xo[e, side - 1, :, :, cols] = o[:n_edge].reshape(side, CORES * cap, n)
            xo[e, close, side - 1, :, cols] = o[n_edge:].reshape(side - 1, CORES * cap, n)
        else:
            xo[e, :, :, :, cols] = o.reshape(side, side, CORES * cap, n)

    def line_ref(h, e, k, span, cols):
        return xo.at[e, spot(k), span, :, cols] if h == 0 else xo.at[e, span, spot(k), :, cols]

    def cols_of(g, h, c):
        return pl.ds(pl.multiple_of(h * half + c * quarter + g * piece, piece), piece)

    def r1_copy(g, h, e, k, span, cm):
        y, x = r1_place(h, k)
        src = line_ref(h, e, k, span, cols_of(g, h, cm))
        return remote(src, mbuf.at[g, h, k, core, e, span], r1_ssem.at[0], r1_rsem.at[g, 0], dev(y, x, cm))

    def r1_partner(g, h, e, span):
        src = line_ref(h, e, 0, span, cols_of(g, h, 1 - core))
        return remote(src, mbuf.at[g, h, 0, core, e, span], r1_ssem.at[1], r1_rsem.at[g, 1], partner)

    n1 = 256

    def up_rows(part, e):
        if part != 'far':
            pltpu.make_async_copy(w13.at[e], w13.at[e], w_sem.at[0, e]).wait()

        def up(t, carry):
            rows = read_rows(part, e)
            cols = pl.ds(t * n1, n1)
            a = jnp.dot(rows, w13[e, 0, :, cols], preferred_element_type=F32)
            b = jnp.dot(rows, w13[e, 1, :, cols], preferred_element_type=F32)
            hid[e % 2, spans[part], cols] = (a * jax.nn.sigmoid(a) * b).astype(BF16)
            return carry

        for t in range(d_expert // n1):
            up(t, 0)

    def send_rows(part, e, g, h):
        for k, span in lines[part][1:]:
            for cm in range(CORES):
                r1_copy(g, h, e, k, span, cm).start()
        span = lines[part][0][1]
        r1_partner(g, h, e, span).start()
        cols = cols_of(g, h, core)
        mbuf[g, h, 0, core, e, span] = xo[e, 0, span, :, cols] if h == 0 else xo[e, span, 0, :, cols]

    def down_group(part, e, g):
        for h in range(2):
            def down(c, carry):
                cols = cols_of(g, h, c)
                write_rows(part, e, cols, jnp.dot(hid[e % 2, spans[part], :], w2[e, :, cols], preferred_element_type=F32).astype(BF16))
                return carry

            for c in range(CORES):
                down(c, 0)
        for h in range(2):
            send_rows(part, e, g, h)

    def wait_down(e):
        pltpu.make_async_copy(w2.at[e], w2.at[e], w_sem.at[1, e]).wait()

    def down_rows(part, e):
        if part != 'far':
            wait_down(e)

        def down(t, carry):
            cols = pl.ds(t * quarter, quarter)
            write_rows(part, e, cols, jnp.dot(hid[e % 2, spans[part], :], w2[e, :, cols], preferred_element_type=F32).astype(BF16))
            return carry

        for h in range(2):
            for t in range(h * CORES, (h + 1) * CORES):
                down(t, 0)
            for g in range(2):
                send_rows(part, e, g, h)

    early = 2

    def far_expert(e, carry):
        up_rows('far', e)
        down_rows('far', e)
        return carry

    def all_expert(e, carry):
        up_rows('all', e)
        wait_down(e)
        down_group('all', e, 0)
        return carry

    def all_second(e, carry):
        down_group('all', e, 1)
        return carry

    up_rows('near', 0)
    land(far, 1)
    down_rows('near', 0)
    land(0, far)
    up_rows('near', 1)
    land(1, far)
    land(side - 1, far)
    down_rows('near', 1)
    land(far, far)
    finish(far, 0)
    finish_near(far)
    lax.fori_loop(0, side, far_lines, 0)
    lax.fori_loop(0, early, far_expert, 0)
    lax.fori_loop(early, local_experts, all_expert, 0)
    lax.fori_loop(early, local_experts, all_second, 0)

    via = 1 + core * (side - 2)
    direct = side - via

    def sum_place(k):
        return lax.div(k + 1, 2)

    def relay_sums(g, h):
        y, x = r2_place(h, via)
        return remote(pbuf.at[g, h, far], rbuf.at[g, h], relay_ssem, relay_rsem.at[g], dev(y, x, core))

    def r2_copy(g, h, k, cd):
        y, x = r2_place(h, k)
        return remote(pbuf.at[g, h, k, cd], ybuf.at[g, h, sum_place(k), core], r2_ssem.at[0], r2_rsem.at[g, 0], dev(y, x, cd))

    def r2_partner(g, h):
        return remote(pbuf.at[g, h, 0, 1 - core], ybuf.at[g, h, 0, core], r2_ssem.at[1], r2_rsem.at[g, 1], partner)

    def merge(g, h, k):
        q = spot(k)
        lhs = []
        for j in range(side):
            span = pl.ds(j * chip_experts, chip_experts)
            hit = slots[h, k, span, :][:, None, :] == wanted[None]
            share = gates[h, k, span, :]
            g_hi = share.astype(BF16).astype(F32)
            g_mid = (share - g_hi).astype(BF16).astype(F32)
            g_lo = share - g_hi - g_mid
            lhs.append(jnp.concatenate([
                jnp.where(hit, v[:, None, :], 0.0).reshape(chip_experts * CORES * cap, LANES).astype(BF16) for v in (g_hi, g_mid, g_lo)], axis=1))
        rows = mbuf[g, h, :, :, :, q].reshape(side * CORES * local_experts * CORES * cap, piece)
        out = lax.dot_general(jnp.concatenate(lhs, axis=0), rows, (((0,), (0,)), ((), ())), preferred_element_type=F32)
        total = out[:LANES] + (out[LANES:2 * LANES] + out[2 * LANES:])
        pbuf[g, h, k] = total.reshape(CORES, num_tokens, piece)

    def wait_bytes(ref, sem):
        pltpu.make_async_copy(ref, ref, sem).wait()

    def pass_on(g):
        wait_bytes(rbuf.at[g], relay_rsem.at[g])
        for h in range(2):
            pbuf[g, h, via] = pbuf[g, h, via] + rbuf[g, h]
            for cd in range(CORES):
                r2_copy(g, h, via, cd).start()

    def merge_group(g, carry):
        wait_bytes(mbuf.at[g, :, pl.ds(1, side - 1)], r1_rsem.at[g, 0])
        wait_bytes(mbuf.at[g, :, 0, 1 - core], r1_rsem.at[g, 1])

        for h in range(2):
            merge(g, h, far)
            relay_sums(g, h).start()

        @pl.when(g > 0)
        def _():
            pass_on(g - 1)

        for h in range(2):
            merge(g, h, direct)
            for cd in range(CORES):
                r2_copy(g, h, direct, cd).start()
        for h in range(2):
            merge(g, h, via)
        for h in range(2):
            merge(g, h, 0)
            r2_partner(g, h).start()
            ybuf[g, h, 0, core] = pbuf[g, h, 0, core]
        return carry

    lax.fori_loop(0, 2, merge_group, 0)
    pass_on(1)

    for g in range(2):
        wait_bytes(ybuf.at[g, :, pl.ds(1, 2)], r2_rsem.at[g, 0])
        wait_bytes(ybuf.at[g, :, 0, 1 - core], r2_rsem.at[g, 1])
        for h in range(2):
            for c in range(CORES):
                total = ybuf[g, h, 0, c]
                for k in range(1, 3):
                    total = total + ybuf[g, h, k, c]
                y_ref[:, cols_of(g, h, c)] = total.astype(BF16)

    for stage in range(3):
        wait_meta(stage, meta_ssem)
    for h in range(2):
        wait_bytes(xg.at[h, pl.ds(0, side - 1 + 2 * side + side + chips)], ag_ssem.at[h])
    wait_bytes(mbuf.at[:, :, pl.ds(1, side - 1)], r1_ssem.at[0])
    wait_bytes(mbuf.at[:, :, 0, 0], r1_ssem.at[1])
    wait_bytes(pbuf.at[:, :, pl.ds(0, 2)], r2_ssem.at[0])
    wait_bytes(rbuf, relay_ssem)
    wait_bytes(pbuf.at[:, :, 0, 0], r2_ssem.at[1])


def solution(mesh):
    num_devices = mesh.shape['ep']
    side = math.isqrt(num_devices // CORES)
    row_spec = P(('dp', 'ep'), None)
    expert_spec = P('ep', None, None)

    def device_step(tokens, routes, w_router, w_one, w_three, w_two):
        num_tokens, d_model = tokens.shape
        top_k = routes.shape[1]
        num_experts = w_router.shape[1]
        local_experts, _, d_expert = w_one.shape
        cap = slot_capacity(num_tokens, top_k, num_experts)
        half = d_model // 2
        piece = half // CORES // 2
        chips = side * side
        any_spec = pl.BlockSpec(memory_space=pl.ANY)
        vmem_spec = pl.BlockSpec(memory_space=pltpu.VMEM)
        dma = pltpu.SemaphoreType.DMA
        return pl.pallas_call(
            functools.partial(moe_kernel, side),
            out_shape=jax.ShapeDtypeStruct((num_tokens, d_model), BF16),
            in_specs=[any_spec, any_spec, any_spec, any_spec, any_spec, any_spec],
            out_specs=vmem_spec,
            scratch_shapes=[
                pltpu.VMEM((2, num_devices, num_tokens, half), BF16),
                pltpu.VMEM((top_k, num_tokens), jnp.int32),
                pltpu.VMEM((d_model, num_experts), BF16),
                pltpu.VMEM((local_experts, 2, d_model, d_expert), BF16),
                pltpu.VMEM((local_experts, d_expert, d_model), BF16),
                pltpu.VMEM((local_experts, side, side, CORES * cap, d_model), BF16),
                pltpu.VMEM((2, chips * CORES * cap, d_expert), BF16),
                pltpu.VMEM((side, side, CORES, top_k, LANES), F32),
                pltpu.VMEM((side, side, CORES * local_experts, LANES), F32),
                pltpu.VMEM((2, side, side * CORES * local_experts, LANES), F32),
                pltpu.VMEM((2, side, side * CORES * local_experts, LANES), F32),
                pltpu.VMEM((2, 2, side, CORES, local_experts, side, CORES * cap, piece), BF16),
                pltpu.VMEM((2, 2, side, CORES, num_tokens, piece), F32),
                pltpu.VMEM((2, 2, CORES, num_tokens, piece), F32),
                pltpu.VMEM((2, 2, 3, CORES, num_tokens, piece), F32),
                dma, dma, dma, dma((2, local_experts)), dma((3,)), dma((3,)), dma((2,)), dma((side, side)), dma((side, side - 1)),
                dma((2,)), dma((2, 2)), dma, dma((2,)), dma((2,)), dma((2, 2)),
            ],
            compiler_params=pltpu.CompilerParams(collective_id=0, has_side_effects=True, vmem_limit_bytes=67043328),
        )(tokens, routes.T, w_router, w_one, w_three, w_two)

    return jax.shard_map(device_step, mesh=mesh, in_specs=(row_spec, row_spec, P(None, None), expert_spec, expert_spec, expert_spec), out_specs=row_spec, check_vma=False)
```

```python
import functools
import math

import jax
import jax.numpy as jnp
from jax import lax
from jax.experimental import pallas as pl
from jax.experimental.pallas import tpu as pltpu
from jax.sharding import PartitionSpec as P

MESH = pl.DeviceIdType.MESH
F32 = jnp.float32
BF16 = jnp.bfloat16
CORES = 2
LANES = 128


def slot_capacity(num_tokens, top_k, num_experts):
    return 8 * ((3 * num_tokens * top_k + 16 * num_experts - 1) // (16 * num_experts))


def moe_kernel(
    side,
    x_hbm, routes_hbm, wr_hbm, w1_hbm, w3_hbm, w2_hbm, y_ref,
    xg, routes_ref, wr, w13, w2, xo, hid, meta, mine, slots, gates, mbuf, pbuf, rbuf, ybuf,
    x_sem, wr_sem, routes_sem, w_sem, meta_ssem, meta_rsem, ag_ssem, ag_rsem, core_rsem,
    r1_ssem, r1_rsem, relay_ssem, relay_rsem, r2_ssem, r2_rsem,
):
    num_devices = CORES * side * side
    chips = side * side
    num_tokens, d_model = x_hbm.shape
    half = d_model // 2
    quarter = half // CORES
    piece = quarter // 2
    local_experts, _, _, d_expert = w13.shape
    chip_experts = CORES * local_experts
    num_experts = num_devices * local_experts
    top_k = routes_ref.shape[0]
    cap = xo.shape[3] // CORES

    me = lax.axis_index('ep')
    core = lax.rem(me, CORES)
    my_x = lax.rem(lax.div(me, CORES), side)
    my_y = lax.div(me, CORES * side)

    def ring(v, k):
        return lax.rem(v + k, side)

    far = side // 2

    def spot(k):
        return k + (k // far) * (side + 1 - 2 * k)

    def chip_at(y, x):
        return y * side + x

    def dev(y, x, c):
        return chip_at(y, x) * CORES + c

    partner = dev(my_y, my_x, 1 - core)

    def remote(src, dst, ssem, rsem, target):
        return pltpu.make_async_remote_copy(src_ref=src, dst_ref=dst, send_sem=ssem, recv_sem=rsem, device_id={'ep': target}, device_id_type=MESH)

    barrier = pltpu.get_barrier_semaphore()

    peers = [partner]
    for k in range(1, side):
        for c in range(CORES):
            peers += [dev(my_y, ring(my_x, k), c), dev(ring(my_y, k), my_x, c)]
    for peer in peers:
        pl.semaphore_signal(barrier, inc=1, device_id={'ep': peer}, device_id_type=MESH)

    x_copies = [pltpu.make_async_copy(x_hbm.at[:, pl.ds(h * half, half)], xg.at[h, me], x_sem) for h in range(2)]
    for cp in x_copies:
        cp.start()
    wr_copy = pltpu.make_async_copy(wr_hbm, wr, wr_sem)
    wr_copy.start()
    routes_copy = pltpu.make_async_copy(routes_hbm, routes_ref, routes_sem)
    routes_copy.start()

    def weight_copies(e):
        return [
            pltpu.make_async_copy(w1_hbm.at[e], w13.at[e, 0], w_sem.at[0, e]),
            pltpu.make_async_copy(w3_hbm.at[e], w13.at[e, 1], w_sem.at[0, e]),
            pltpu.make_async_copy(w2_hbm.at[e], w2.at[e], w_sem.at[1, e]),
        ]

    def start_weights(e, carry):
        for cp in weight_copies(e):
            cp.start()
        return carry

    lax.fori_loop(0, local_experts, start_weights, 0)


    pltpu.make_async_copy(xg.at[:, me], xg.at[:, me], x_sem).wait()

    pl.semaphore_wait(barrier, len(peers))

    def place(h, a, b):
        if h == 0:
            return ring(my_y, b), ring(my_x, a)
        return ring(my_y, a), ring(my_x, b)

    def block_src(h, a, b, c):
        y, x = place(h, a, b)
        return dev(y, x, c)

    def move_block(h, src, rsem, target):
        return remote(xg.at[h, src], xg.at[h, src], ag_ssem.at[h], rsem, target)

    def first_copy(h, k):
        return move_block(h, me, ag_rsem.at[side - k, 0], block_src(h, k, 0, core))

    def first_relay(h):
        k = 1 + core * (side - 2)
        return move_block(h, block_src(h, k, 0, core), ag_rsem.at[side // 2, 0], block_src(h, side - k, 0, core))

    def second_copy(h, a, k):
        return move_block(h, block_src(h, a, 0, core), ag_rsem.at[a, side - k], block_src(h, 0, k, core))

    def relay_copy(h, a, k):
        return move_block(h, block_src(h, a, k, core), ag_rsem.at[a, side // 2], block_src(h, 0, side - k, core))

    def core_copy(h, a, b):
        return move_block(h, block_src(h, a, b, core), core_rsem.at[a, 1 if b == side - 1 else b], partner)

    def wait_blocks(sem):
        pltpu.make_async_copy(xg.at[:, me], xg.at[:, me], sem).wait()

    def meta_copy(stage, k):
        ref = (meta.at[my_y, my_x, core], meta.at[my_y, :, core], meta.at[:, :, core])[stage]
        target = (dev(my_y, ring(my_x, k), core), dev(ring(my_y, k), my_x, core), partner)[stage]
        return remote(ref, ref, meta_ssem.at[stage], meta_rsem.at[stage], target)

    def wait_meta(stage, sem):
        ref = (meta.at[0, pl.ds(0, side - 1), 0], meta.at[pl.ds(0, side - 1), :, 0], meta.at[:, :, 0])[stage]
        pltpu.make_async_copy(ref, ref, sem.at[stage]).wait()

    for h in range(2):
        for k in (1, side - 1):
            first_copy(h, k).start()

    wr_copy.wait()
    routes_copy.wait()
    x_local = [xg[h, me] for h in range(2)]
    logits = sum(
        lax.dot_general(wr[pl.ds(h * half, half), :], x_local[h], (((0,), (1,)), ((), ())), preferred_element_type=F32)
        for h in range(2)
    )
    routes = routes_ref[...]
    expert_iota = lax.broadcasted_iota(jnp.int32, (num_experts, num_tokens), 0)
    picked = jnp.concatenate(
        [jnp.sum(jnp.where(expert_iota == routes[j:j + 1, :], logits, 0.0), axis=0, keepdims=True) for j in range(top_k)], axis=0)
    ex = jnp.exp(picked - jnp.max(picked, axis=0, keepdims=True))
    gate = ex / jnp.sum(ex, axis=0, keepdims=True)
    meta[my_y, my_x, core] = jnp.concatenate([routes.astype(F32) + 1.0, gate], axis=1)

    for k in range(1, side):
        meta_copy(0, k).start()
    for h in range(2):
        for k in (1, side - 1):
            second_copy(h, 0, k).start()
        core_copy(h, 0, 0).start()

    row_i = lax.broadcasted_iota(jnp.int32, (LANES, LANES), 0)
    col_i = lax.broadcasted_iota(jnp.int32, (LANES, LANES), 1)
    before = jnp.where((row_i < col_i) & (row_i // num_tokens == col_i // num_tokens), 1.0, 0.0).astype(BF16)
    tile_ids = lax.broadcasted_iota(jnp.int32, (chip_experts, LANES), 0) + 1

    def chip_ids(y, x):
        return (tile_ids + chip_at(y, x) * chip_experts).astype(F32)

    def chip_routes(y, x):
        tiles = [meta[y, x, c] for c in range(CORES)]
        turned = [pltpu.roll(v, num_tokens, 1) for v in tiles]
        low = lax.broadcasted_iota(jnp.int32, tiles[0].shape, 1) < num_tokens
        return jnp.where(low, tiles[0], turned[1]), jnp.where(low, turned[0], tiles[1])

    def slots_of(mask):
        rank = jnp.dot(mask.astype(BF16), before, preferred_element_type=F32)
        return jnp.where(mask > 0.0, rank, -1.0)

    my_ids = chip_ids(my_y, my_x)

    def plan_gather(y, carry):
        for x in range(side):
            picks, _ = chip_routes(y, x)
            mask = jnp.zeros((chip_experts, LANES), F32)
            for j in range(top_k):
                mask = jnp.where(my_ids == picks[j:j + 1, :], 1.0, mask)
            mine[y, x] = mask
        return carry

    def plan_merge(k, carry):
        for h in range(2):
            ids = jnp.concatenate([chip_ids(*r1_place(h, side - j)) for j in range(side)], axis=0)
            picks, shares = chip_routes(*r2_place(h, k))
            mask = jnp.zeros(ids.shape, F32)
            weight = jnp.zeros(ids.shape, F32)
            for j in range(top_k):
                hit = ids == picks[j:j + 1, :]
                mask = jnp.where(hit, 1.0, mask)
                weight = jnp.where(hit, shares[j:j + 1, :], weight)
            slots[h, k] = slots_of(mask)
            gates[h, k] = weight
        return carry

    def r1_place(h, k):
        if h == 0:
            return ring(my_y, k), my_x
        return my_y, ring(my_x, k)

    def r2_place(h, k):
        if h == 0:
            return my_y, ring(my_x, k)
        return ring(my_y, k), my_x

    pair_row = lax.broadcasted_iota(jnp.int32, (CORES * cap, LANES), 0)
    pair_lane = lax.broadcasted_iota(jnp.int32, (CORES * cap, LANES), 1)
    wanted = jnp.where(pair_row // cap == pair_lane // num_tokens, pair_row % cap, -2).astype(F32)

    def gather_chip(h, a, b):
        p = chip_at(*place(h, a, b))
        py, px = (spot(b), spot(a)) if h == 0 else (spot(a), spot(b))
        found = mine[place(h, a, b)[0], place(h, a, b)[1], pl.ds(core * local_experts, local_experts), :]
        pick = jnp.where(found[:, None, :] == wanted[None], 1.0, 0.0).reshape(local_experts * CORES * cap, LANES).astype(BF16)
        rows = xg[h, pl.ds(p * CORES, CORES)].reshape(CORES * num_tokens, half)
        out = jnp.dot(pick, rows, preferred_element_type=F32).astype(BF16)
        xo[:, py, px, :, pl.ds(h * half, half)] = out.reshape(local_experts, CORES * cap, half)

    def pick_rows(a, b):
        for h in range(2):
            gather_chip(h, a, b)

    def finish(a, b):
        wait_blocks(core_rsem.at[a, b])
        pick_rows(a, b)

    def finish_near(a):
        four = xg.at[:, pl.ds(0, 2)]
        pltpu.make_async_copy(four, four, core_rsem.at[a, 1]).wait()
        pick_rows(a, 1)
        pick_rows(a, side - 1)

    def arrive(a, b):
        wait_blocks(ag_rsem.at[a, b])

    def share(a, b):
        for h in range(2):
            core_copy(h, a, b).start()

    def land(a, b):
        arrive(a, b)
        share(a, b)

    near = (1, side - 1) + tuple(range(2, side - 1))

    def same_line(a):
        for h in range(2):
            for k in (1, side - 1):
                second_copy(h, a, k).start()

    def relay(a, k):
        for h in range(2):
            relay_copy(h, a, k).start()

    def own_lines(p, carry):
        finish(spot(p), 0)
        return carry

    def near_lines(p, carry):
        finish_near(spot(p))
        return carry

    def far_lines(p, carry):
        finish(spot(p), far)
        return carry

    for a in near[:2]:
        arrive(a, 0)
    for h in range(2):
        first_relay(h).start()
    wait_meta(0, meta_rsem)
    for k in range(1, side):
        meta_copy(1, k).start()
    for a in near[:2]:
        same_line(a)
    for a in near[:2]:
        share(a, 0)
    arrive(0, 1)
    relay(0, 1)
    share(0, 1)
    land(0, side - 1)
    arrive(far, 0)
    same_line(far)
    share(far, 0)
    wait_meta(1, meta_rsem)
    meta_copy(2, 0).start()
    wait_meta(2, meta_rsem)
    lax.fori_loop(0, side, plan_gather, 0)
    mine[...] = slots_of(mine[...].reshape(chips * chip_experts, LANES)).reshape(side, side, chip_experts, LANES)
    lax.fori_loop(0, side, plan_merge, 0)
    arrive(1, 1)
    relay(1, 1)
    share(1, 1)
    arrive(side - 1, side - 1)
    relay(side - 1, side - 1)
    share(side - 1, side - 1)
    land(1, side - 1)
    land(side - 1, 1)
    lax.fori_loop(0, side - 1, own_lines, 0)
    lax.fori_loop(0, side - 1, near_lines, 0)
    arrive(far, side - 1)
    relay(far, side - 1)
    share(far, side - 1)

    close, edge = pl.ds(0, side - 1), pl.ds(side - 1, 1)
    whole = pl.ds(0, side)
    n_close = (side - 1) * (side - 1) * CORES * cap
    n_rows = chips * CORES * cap
    lines = {
        'near': [(0, close)] + [(k, close) for k in (1, side - 1)],
        'far': [(0, edge)] + [(far, whole)] + [(k, edge) for k in (1, side - 1)],
        'all': [(0, whole)] + [(k, whole) for k in (far, 1, side - 1)],
    }
    spans = {'near': pl.ds(0, n_close), 'far': pl.ds(n_close, n_rows - n_close), 'all': pl.ds(0, n_rows)}

    def read_rows(part, e):
        if part == 'near':
            return xo[e, close, close].reshape(n_close, d_model)
        if part == 'far':
            n_edge = side * CORES * cap
            return jnp.concatenate([xo[e, side - 1].reshape(n_edge, d_model), xo[e, close, side - 1].reshape(n_rows - n_close - n_edge, d_model)], axis=0)
        return xo[e].reshape(n_rows, d_model)

    def write_rows(part, e, cols, o):
        n = o.shape[1]
        if part == 'near':
            xo[e, close, close, :, cols] = o.reshape(side - 1, side - 1, CORES * cap, n)
        elif part == 'far':
            n_edge = side * CORES * cap
            xo[e, side - 1, :, :, cols] = o[:n_edge].reshape(side, CORES * cap, n)
            xo[e, close, side - 1, :, cols] = o[n_edge:].reshape(side - 1, CORES * cap, n)
        else:
            xo[e, :, :, :, cols] = o.reshape(side, side, CORES * cap, n)

    def line_ref(h, e, k, span, cols):
        return xo.at[e, spot(k), span, :, cols] if h == 0 else xo.at[e, span, spot(k), :, cols]

    def cols_of(g, h, c):
        return pl.ds(pl.multiple_of(h * half + c * quarter + g * piece, piece), piece)

    def r1_copy(g, h, e, k, span, cm):
        y, x = r1_place(h, k)
        src = line_ref(h, e, k, span, cols_of(g, h, cm))
        return remote(src, mbuf.at[g, h, k, core, e, span], r1_ssem.at[0], r1_rsem.at[g, 0], dev(y, x, cm))

    def r1_partner(g, h, e, span):
        src = line_ref(h, e, 0, span, cols_of(g, h, 1 - core))
        return remote(src, mbuf.at[g, h, 0, core, e, span], r1_ssem.at[1], r1_rsem.at[g, 1], partner)

    n1 = 256

    def up_rows(part, e):
        if part != 'far':
            pltpu.make_async_copy(w13.at[e], w13.at[e], w_sem.at[0, e]).wait()

        def up(t, carry):
            rows = read_rows(part, e)
            cols = pl.ds(t * n1, n1)
            a = jnp.dot(rows, w13[e, 0, :, cols], preferred_element_type=F32)
            b = jnp.dot(rows, w13[e, 1, :, cols], preferred_element_type=F32)
            hid[e % 2, spans[part], cols] = (a * jax.nn.sigmoid(a) * b).astype(BF16)
            return carry

        for t in range(d_expert // n1):
            up(t, 0)

    def send_rows(part, e, g, h):
        for k, span in lines[part][1:]:
            for cm in range(CORES):
                r1_copy(g, h, e, k, span, cm).start()
        span = lines[part][0][1]
        r1_partner(g, h, e, span).start()
        cols = cols_of(g, h, core)
        mbuf[g, h, 0, core, e, span] = xo[e, 0, span, :, cols] if h == 0 else xo[e, span, 0, :, cols]

    def down_group(part, e, g):
        for h in range(2):
            def down(c, carry):
                cols = cols_of(g, h, c)
                write_rows(part, e, cols, jnp.dot(hid[e % 2, spans[part], :], w2[e, :, cols], preferred_element_type=F32).astype(BF16))
                return carry

            for c in range(CORES):
                down(c, 0)
        for h in range(2):
            send_rows(part, e, g, h)

    def wait_down(e):
        pltpu.make_async_copy(w2.at[e], w2.at[e], w_sem.at[1, e]).wait()

    def down_rows(part, e):
        if part != 'far':
            wait_down(e)

        def down(t, carry):
            cols = pl.ds(t * quarter, quarter)
            write_rows(part, e, cols, jnp.dot(hid[e % 2, spans[part], :], w2[e, :, cols], preferred_element_type=F32).astype(BF16))
            return carry

        for h in range(2):
            for t in range(h * CORES, (h + 1) * CORES):
                down(t, 0)
            for g in range(2):
                send_rows(part, e, g, h)

    early = 2

    def far_expert(e, carry):
        up_rows('far', e)
        down_rows('far', e)
        return carry

    def all_expert(e, carry):
        up_rows('all', e)
        wait_down(e)
        down_group('all', e, 0)
        return carry

    def all_second(e, carry):
        down_group('all', e, 1)
        return carry

    up_rows('near', 0)
    land(far, 1)
    down_rows('near', 0)
    land(0, far)
    up_rows('near', 1)
    land(1, far)
    land(side - 1, far)
    down_rows('near', 1)
    land(far, far)
    finish(far, 0)
    finish_near(far)
    lax.fori_loop(0, side, far_lines, 0)
    lax.fori_loop(0, early, far_expert, 0)
    lax.fori_loop(early, local_experts, all_expert, 0)
    lax.fori_loop(early, local_experts, all_second, 0)

    via = 1 + core * (side - 2)
    direct = side - via

    def sum_place(k):
        return lax.div(k + 1, 2)

    def relay_sums(g, h):
        y, x = r2_place(h, via)
        return remote(pbuf.at[g, h, far], rbuf.at[g, h], relay_ssem, relay_rsem.at[g], dev(y, x, core))

    def r2_copy(g, h, k, cd):
        y, x = r2_place(h, k)
        return remote(pbuf.at[g, h, k, cd], ybuf.at[g, h, sum_place(k), core], r2_ssem.at[0], r2_rsem.at[g, 0], dev(y, x, cd))

    def r2_partner(g, h):
        return remote(pbuf.at[g, h, 0, 1 - core], ybuf.at[g, h, 0, core], r2_ssem.at[1], r2_rsem.at[g, 1], partner)

    def merge(g, h, k):
        q = spot(k)
        lhs = []
        for j in range(side):
            span = pl.ds(j * chip_experts, chip_experts)
            hit = slots[h, k, span, :][:, None, :] == wanted[None]
            share = gates[h, k, span, :]
            g_hi = share.astype(BF16).astype(F32)
            g_mid = (share - g_hi).astype(BF16).astype(F32)
            g_lo = share - g_hi - g_mid
            lhs.append(jnp.concatenate([
                jnp.where(hit, v[:, None, :], 0.0).reshape(chip_experts * CORES * cap, LANES).astype(BF16) for v in (g_hi, g_mid, g_lo)], axis=1))
        rows = mbuf[g, h, :, :, :, q].reshape(side * CORES * local_experts * CORES * cap, piece)
        out = lax.dot_general(jnp.concatenate(lhs, axis=0), rows, (((0,), (0,)), ((), ())), preferred_element_type=F32)
        total = out[:LANES] + (out[LANES:2 * LANES] + out[2 * LANES:])
        pbuf[g, h, k] = total.reshape(CORES, num_tokens, piece)

    def wait_bytes(ref, sem):
        pltpu.make_async_copy(ref, ref, sem).wait()

    def pass_on(g):
        wait_bytes(rbuf.at[g], relay_rsem.at[g])
        for h in range(2):
            pbuf[g, h, via] = pbuf[g, h, via] + rbuf[g, h]
            for cd in range(CORES):
                r2_copy(g, h, via, cd).start()

    def merge_group(g, carry):
        wait_bytes(mbuf.at[g, :, pl.ds(1, side - 1)], r1_rsem.at[g, 0])
        wait_bytes(mbuf.at[g, :, 0, 1 - core], r1_rsem.at[g, 1])

        for h in range(2):
            merge(g, h, far)
            relay_sums(g, h).start()

        for h in range(2):
            merge(g, h, direct)
            for cd in range(CORES):
                r2_copy(g, h, direct, cd).start()

        @pl.when(g > 0)
        def _():
            pass_on(g - 1)

        for h in range(2):
            merge(g, h, via)
        for h in range(2):
            merge(g, h, 0)
            r2_partner(g, h).start()
            ybuf[g, h, 0, core] = pbuf[g, h, 0, core]
        return carry

    lax.fori_loop(0, 2, merge_group, 0)
    pass_on(1)

    for g in range(2):
        wait_bytes(ybuf.at[g, :, pl.ds(1, 2)], r2_rsem.at[g, 0])
        wait_bytes(ybuf.at[g, :, 0, 1 - core], r2_rsem.at[g, 1])
        for h in range(2):
            for c in range(CORES):
                total = ybuf[g, h, 0, c]
                for k in range(1, 3):
                    total = total + ybuf[g, h, k, c]
                y_ref[:, cols_of(g, h, c)] = total.astype(BF16)

    for stage in range(3):
        wait_meta(stage, meta_ssem)
    for h in range(2):
        wait_bytes(xg.at[h, pl.ds(0, side - 1 + 2 * side + side + chips)], ag_ssem.at[h])
    wait_bytes(mbuf.at[:, :, pl.ds(1, side - 1)], r1_ssem.at[0])
    wait_bytes(mbuf.at[:, :, 0, 0], r1_ssem.at[1])
    wait_bytes(pbuf.at[:, :, pl.ds(0, 2)], r2_ssem.at[0])
    wait_bytes(rbuf, relay_ssem)
    wait_bytes(pbuf.at[:, :, 0, 0], r2_ssem.at[1])


def solution(mesh):
    num_devices = mesh.shape['ep']
    side = math.isqrt(num_devices // CORES)
    row_spec = P(('dp', 'ep'), None)
    expert_spec = P('ep', None, None)

    def device_step(tokens, routes, w_router, w_one, w_three, w_two):
        num_tokens, d_model = tokens.shape
        top_k = routes.shape[1]
        num_experts = w_router.shape[1]
        local_experts, _, d_expert = w_one.shape
        cap = slot_capacity(num_tokens, top_k, num_experts)
        half = d_model // 2
        piece = half // CORES // 2
        chips = side * side
        any_spec = pl.BlockSpec(memory_space=pl.ANY)
        vmem_spec = pl.BlockSpec(memory_space=pltpu.VMEM)
        dma = pltpu.SemaphoreType.DMA
        return pl.pallas_call(
            functools.partial(moe_kernel, side),
            out_shape=jax.ShapeDtypeStruct((num_tokens, d_model), BF16),
            in_specs=[any_spec, any_spec, any_spec, any_spec, any_spec, any_spec],
            out_specs=vmem_spec,
            scratch_shapes=[
                pltpu.VMEM((2, num_devices, num_tokens, half), BF16),
                pltpu.VMEM((top_k, num_tokens), jnp.int32),
                pltpu.VMEM((d_model, num_experts), BF16),
                pltpu.VMEM((local_experts, 2, d_model, d_expert), BF16),
                pltpu.VMEM((local_experts, d_expert, d_model), BF16),
                pltpu.VMEM((local_experts, side, side, CORES * cap, d_model), BF16),
                pltpu.VMEM((2, chips * CORES * cap, d_expert), BF16),
                pltpu.VMEM((side, side, CORES, top_k, LANES), F32),
                pltpu.VMEM((side, side, CORES * local_experts, LANES), F32),
                pltpu.VMEM((2, side, side * CORES * local_experts, LANES), F32),
                pltpu.VMEM((2, side, side * CORES * local_experts, LANES), F32),
                pltpu.VMEM((2, 2, side, CORES, local_experts, side, CORES * cap, piece), BF16),
                pltpu.VMEM((2, 2, side, CORES, num_tokens, piece), F32),
                pltpu.VMEM((2, 2, CORES, num_tokens, piece), F32),
                pltpu.VMEM((2, 2, 3, CORES, num_tokens, piece), F32),
                dma, dma, dma, dma((2, local_experts)), dma((3,)), dma((3,)), dma((2,)), dma((side, side)), dma((side, side - 1)),
                dma((2,)), dma((2, 2)), dma, dma((2,)), dma((2,)), dma((2, 2)),
            ],
            compiler_params=pltpu.CompilerParams(collective_id=0, has_side_effects=True, vmem_limit_bytes=67043328),
        )(tokens, routes.T, w_router, w_one, w_three, w_two)

    return jax.shard_map(device_step, mesh=mesh, in_specs=(row_spec, row_spec, P(None, None), expert_spec, expert_spec, expert_spec), out_specs=row_spec, check_vma=False)
```
